32 devices in a mesh: row: 16 (over z, x, core), col: 2 (over y).
Axes of the slice: x: 2, y: 2, z: 4, core: 2. Of those that a mesh axis runs over, the one named last changes fastest.
Arguments:
- features: bfloat16 [16384, 512], P(('row', 'col')), may hold values from -6 to 6
- factor: float32 [16384, 1024], P(('row', 'col')), may hold values from -0.03 to 0.03
- ip_weights: float32 [16384], P(('row', 'col')), may hold values from 0.1 to 30
- pivot_owner: int32 [256], replicated, may hold values from 0 to 31, as said below
- pivot_position: int32 [256], replicated, may hold values from 0 to 511, as said below
Outputs:
- new_columns: float32 [16384, 256], P(('row', 'col'))
- gram_rows: float32 [256, 1280], replicated
The draws below stay inside these ranges and needn't reach their ends.
Inputs may be any that keep to these rules, and one draw needn't show every extreme that they name: `pivot_owner`: each device owns at most 18 pivots, and some device owns exactly 18. `pivot_position`: pivots with the same owner have different positions.
All inputs are finite; a program needn't handle non-finite values.
Results may differ from the reference program's by a relative error of at most 0.0003.
Values may be sent and summed in bfloat16 or wider, within the bound.
No kernel may reach another device: no remote copies, remote signals or barrier semaphores. Data moves between devices by JAX's collectives and lax.ppermute only.
A program may use at most 64 MiB of HBM per device.

```python
import math
import jax
import jax.numpy as jnp
from jax import lax

F = 512
R = 1024
B = 256
ROWS_DEV = 512
SAMPLES = 16384
PIV_MOST = 18
DEVICES = 32


def pivot_layout(key):
    base = jax.random.fold_in(key, 7)
    key_sizes, key_devices, key_perm, key_shift = jax.random.split(base, 4)
    least = max(1, PIV_MOST // 2)
    group_sizes = jax.random.randint(key_sizes, (B,), least, PIV_MOST + 1).at[0].set(PIV_MOST)
    group_ends = jnp.cumsum(group_sizes)
    pivot_index = jnp.arange(B)
    group_of = jnp.sum((group_ends[None, :] <= pivot_index[:, None]).astype(jnp.int32), axis=1)
    group_start = jnp.where(group_of > 0, group_ends[jnp.maximum(group_of - 1, 0)], 0)
    within = pivot_index - group_start
    devices_perm = jax.random.permutation(key_devices, DEVICES)
    owner_ids = devices_perm[group_of]
    row_perm = jax.random.permutation(key_perm, ROWS_DEV)
    shifts = jax.random.randint(key_shift, (B,), 0, ROWS_DEV)
    positions = row_perm[(within + shifts[group_of]) % ROWS_DEV]
    return (owner_ids.astype(jnp.int32), positions.astype(jnp.int32))


def draw_pivot_owner(key, part):
    return pivot_layout(key)[0]


def draw_pivot_position(key, part):
    return pivot_layout(key)[1]


def draw_ip_weights(key, part):
    base = jax.random.fold_in(key, 23)
    rising = 1.0 + 2.0 * jnp.arange(SAMPLES, dtype=jnp.float32) / max(SAMPLES - 1, 1)
    level = jnp.exp(jax.random.uniform(base, (SAMPLES,), jnp.float32, math.log(0.1), math.log(10.0)))
    return level * rising


def draw_features(key, part):
    base = jax.random.fold_in(key, 31)
    values = jnp.clip(jax.random.normal(base, (SAMPLES, F), jnp.float32), -6.0, 6.0)
    return values.astype(jnp.bfloat16)


def draw_factor(key, part):
    base = jax.random.fold_in(key, 41)
    spread = 0.01
    values = jnp.clip(spread * jax.random.normal(base, (SAMPLES, R), jnp.float32), -3.0 * spread, 3.0 * spread)
    return values


def setup_inputs(seed: int = 0) -> dict:
    keys = jax.random.split(jax.random.key(seed), 6)
    return {
        "features": draw_features(jax.random.fold_in(keys[5], 71), 0),
        "factor": draw_factor(jax.random.fold_in(keys[5], 71), 0),
        "ip_weights": draw_ip_weights(jax.random.fold_in(keys[5], 71), 0),
        "pivot_owner": draw_pivot_owner(jax.random.fold_in(keys[5], 71), 0),
        "pivot_position": draw_pivot_position(jax.random.fold_in(keys[5], 71), 0),
    }


kernel_rates = (0.25, 0.5, 1.0)
kernel_mixes = (0.5, 0.3, 0.2)

def kernel_of(left, right):
    cross_term = jnp.dot(left.astype(jnp.float32), right.T.astype(jnp.float32), preferred_element_type=jnp.float32)
    left_norms = jnp.sum(jnp.square(left.astype(jnp.float32)), axis=1)
    right_norms = jnp.sum(jnp.square(right.astype(jnp.float32)), axis=1)
    distance = left_norms[:, None] + right_norms[None, :] - 2.0 * cross_term
    total = jnp.zeros_like(distance)
    for rate, mixing in zip(kernel_rates, kernel_mixes):
        total = total + mixing * jnp.exp(-(rate / F) * distance)
    return total

def reference(features, factor, ip_weights, pivot_owner, pivot_position):
    chosen = (pivot_owner * ROWS_DEV + pivot_position).astype(jnp.int32)
    pivot_x = features[chosen]
    pivot_h = factor[chosen]
    residual = kernel_of(features, pivot_x) - jnp.dot(factor, pivot_h.T, precision=lax.Precision.HIGHEST)
    block = kernel_of(pivot_x, pivot_x) - jnp.dot(pivot_h, pivot_h.T, precision=lax.Precision.HIGHEST)
    lower_block = jnp.linalg.cholesky(block)
    new_columns = jax.scipy.linalg.solve_triangular(lower_block, residual.T, lower=True).T
    weighted = new_columns * ip_weights[:, None]
    left_part = jnp.dot(weighted.T, factor, precision=lax.Precision.HIGHEST)
    right_part = jnp.dot(weighted.T, new_columns, precision=lax.Precision.HIGHEST)
    gram_rows = jnp.concatenate([left_part, right_part], axis=1) / SAMPLES
    return (new_columns, gram_rows)
```

```python
import jax
import jax.numpy as jnp
from jax import lax
from jax.experimental import pallas as pl
from jax.experimental.pallas import tpu as pltpu
from jax.sharding import PartitionSpec as P

HIGHEST = lax.Precision.HIGHEST
f32 = jnp.float32
bf16 = jnp.bfloat16


def nt(a, b, precision=None):
    return lax.dot_general(a, b, (((1,), (1,)), ((), ())), precision=precision, preferred_element_type=f32)


def tn(a, b, precision=None):
    return lax.dot_general(a, b, (((0,), (0,)), ((), ())), precision=precision, preferred_element_type=f32)


def nn(a, b, precision=None):
    return lax.dot_general(a, b, (((1,), (0,)), ((), ())), precision=precision, preferred_element_type=f32)


def split(a):
    high = a.astype(bf16)
    low = (a - high.astype(f32)).astype(bf16)
    return high, low


def call(kernel, outs, *args, smem=0, scratch=(), flops=10**8):
    specs = [pl.BlockSpec(memory_space=pltpu.SMEM)] * smem + [
        pl.BlockSpec(memory_space=pltpu.VMEM)
    ] * (len(args) - smem)
    return pl.pallas_call(
        kernel,
        out_shape=outs,
        in_specs=specs,
        out_specs=jax.tree.map(lambda _: pl.BlockSpec(memory_space=pltpu.VMEM), outs),
        scratch_shapes=scratch,
        cost_estimate=pl.CostEstimate(flops=flops, transcendentals=0, bytes_accessed=10**6),
    )(*args)


def pick_kernel(rank_ref, owner_ref, position_ref, features_ref, factor_ref, slots_ref):
    slots = slots_ref.shape[0]
    pivots = owner_ref.shape[1]
    rows = features_ref.shape[0]
    width = features_ref.shape[1]
    depth = factor_ref.shape[1]
    mine = owner_ref[...] == rank_ref[0]
    ahead = lax.broadcasted_iota(jnp.int32, (pivots, pivots), 0) < lax.broadcasted_iota(
        jnp.int32, (pivots, pivots), 1
    )
    mine_rows = jnp.broadcast_to(jnp.where(mine, 1.0, 0.0), (8, pivots)).astype(bf16)
    order = nn(mine_rows, jnp.where(ahead, 1.0, 0.0).astype(bf16))[0:1, :].astype(jnp.int32)
    slot = lax.broadcasted_iota(jnp.int32, (slots, pivots), 0)
    chosen = jnp.where((slot == order) & mine, 1.0, 0.0).astype(bf16)
    sample = lax.broadcasted_iota(jnp.int32, (rows, pivots), 0)
    located = jnp.where(sample == position_ref[...], 1.0, 0.0).astype(bf16)
    take = nt(chosen, located).astype(bf16)
    high, low = split(factor_ref[...])
    slots_ref[:, 0:width] = nn(take, features_ref[...]).astype(bf16)
    slots_ref[:, width : width + depth] = nn(take, high).astype(bf16)
    slots_ref[:, width + depth : width + 2 * depth] = nn(take, low).astype(bf16)


def mixed(cross, left, right, width):
    base = jnp.exp((left + right - 2.0 * cross) * (-0.25 / width))
    square = base * base
    return 0.5 * base + 0.3 * square + 0.2 * (square * square)


def residual_kernel(
    me_ref, source_ref, near_ref, far_ref, features_ref, factor_ref, weights_ref,
    residual_ref, block_ref, send_ref, keep_ref,
):
    pivots = source_ref.shape[0]
    held = near_ref.shape[0]
    width = features_ref.shape[1]
    depth = factor_ref.shape[1]
    place = lax.broadcasted_iota(jnp.int32, (pivots, held), 1)
    source = source_ref[...]
    from_near = jnp.where(place == source, 1.0, 0.0).astype(bf16)
    from_far = jnp.where(place == source - held, 1.0, 0.0).astype(bf16)
    pivot = (nn(from_near, near_ref[...]) + nn(from_far, far_ref[...])).astype(bf16)
    pivot_x = pivot[:, 0:width]
    pivot_hi = pivot[:, width : width + depth]
    pivot_lo = pivot[:, width + depth :]
    features = features_ref[...]
    factor = factor_ref[...]
    high, low = split(factor)
    wide = features.astype(f32)
    pivot_wide = pivot_x.astype(f32)
    left = jnp.sum(wide * wide, axis=1, keepdims=True)
    pivot_square = pivot_wide * pivot_wide
    pivot_left = jnp.sum(pivot_square, axis=1, keepdims=True)
    right = nt(jnp.ones((8, width), f32), pivot_square, HIGHEST)[0:1, :]
    product = nt(high, pivot_hi) + (nt(low, pivot_hi) + nt(high, pivot_lo))
    residual = mixed(nt(features, pivot_x), left, right, width) - product
    residual_ref[...] = residual
    pivot_product = nt(pivot_hi, pivot_hi) + (nt(pivot_lo, pivot_hi) + nt(pivot_hi, pivot_lo))
    block_ref[...] = mixed(nt(pivot_x, pivot_x), pivot_left, right, width) - pivot_product
    weighted = residual * weights_ref[...]
    gram_left = tn(weighted, factor, HIGHEST)
    gram_right = tn(weighted, residual, HIGHEST)
    half = keep_ref.shape[0]
    piece = keep_ref.shape[1]
    for p in range(2 * half):
        near, far = me_ref[0] ^ p, me_ref[1] ^ p

        @pl.when(near < half)
        def _():
            keep_ref[near, :, 0:depth] = gram_left[p * piece : (p + 1) * piece, :]
            keep_ref[near, :, depth:] = gram_right[p * piece : (p + 1) * piece, :]

        @pl.when(far < half)
        def _():
            send_ref[far, :, 0:depth] = gram_left[p * piece : (p + 1) * piece, :]
            send_ref[far, :, depth:] = gram_right[p * piece : (p + 1) * piece, :]


def inverse_kernel(block_ref, out_ref, work_ref):
    n = block_ref.shape[0]
    size = 32
    work_ref[...] = block_ref[...]
    lane = lax.broadcasted_iota(jnp.int32, (size, n), 1)
    row_wide = lax.broadcasted_iota(jnp.int32, (size, n), 0)
    row = lax.broadcasted_iota(jnp.int32, (size, 128), 0)
    full_lane = lax.broadcasted_iota(jnp.int32, (n, n), 1)
    full_row = lax.broadcasted_iota(jnp.int32, (n, n), 0)

    def panel(k, carry):
        first = pl.multiple_of(k * size, size)
        rows = work_ref[pl.ds(first, size), :]
        slab = rows[:, 0:128]
        for g in range(1, n // 128):
            slab = jnp.where(first >= g * 128, rows[:, g * 128 : (g + 1) * 128], slab)
        slab = pltpu.roll(slab, (128 - first % 128) % 128, 1)
        columns = [jnp.broadcast_to(slab[:, j : j + 1], (size, 128)) for j in range(size)]
        scale = jnp.zeros((size, 128), f32)
        for j in range(size):
            pivot = columns[j][j : j + 1, :]
            scale = jnp.where(row == j, lax.rsqrt(pivot), scale)
            factor = jnp.where(row > j, columns[j] * (1.0 / pivot), 0.0)
            for l in range(j + 1, size):
                columns[l] = columns[l] - factor * columns[l][j : j + 1, :]
            rows = jnp.where(lane == first + j, jnp.where(row_wide == j, 1.0, 0.0), rows)
            rows = rows - jnp.concatenate([factor] * (n // 128), axis=1) * rows[j : j + 1, :]
        rows = rows * jnp.concatenate([scale] * (n // 128), axis=1)
        upper = jnp.where(lane >= first + size, rows, 0.0)
        update = tn(upper, rows, HIGHEST)
        stale = (full_row >= first + size) & (full_lane >= first) & (full_lane < first + size)
        work_ref[...] = jnp.where(stale, 0.0, work_ref[...]) - update
        work_ref[pl.ds(first, size), :] = rows
        return carry

    lax.fori_loop(0, n // size, panel, 0)
    out_ref[...] = jnp.where(full_lane <= full_row, work_ref[...], 0.0)


def columns_kernel(residual_ref, inverse_ref, out_ref):
    out_ref[...] = nt(residual_ref[...], inverse_ref[...], HIGHEST)


def rows_kernel(me_ref, near_ref, far_ref, inverse_ref, out_ref, work_ref):
    half = near_ref.shape[0]
    piece = near_ref.shape[1]
    n = inverse_ref.shape[0]
    depth = out_ref.shape[1] - n
    for p in range(2 * half):
        near, far = me_ref[0] ^ p, me_ref[1] ^ p

        @pl.when(near < half)
        def _():
            work_ref[p * piece : (p + 1) * piece, :] = near_ref[near]

        @pl.when(far < half)
        def _():
            work_ref[p * piece : (p + 1) * piece, :] = far_ref[far]

    inverse = inverse_ref[...]
    out_ref[:, 0:depth] = nn(inverse, work_ref[:, 0:depth], HIGHEST)
    out_ref[:, depth:] = nt(nn(inverse, work_ref[:, depth:], HIGHEST), inverse, HIGHEST)


def bits(value, low, count):
    return [(value >> (low + k)) & 1 for k in range(count)]


def body(features, factor, ip_weights, pivot_owner, pivot_position):
    axes = ("row", "col")
    n_row, n_col = lax.axis_size("row"), lax.axis_size("col")
    devices = n_row * n_col
    row_bits, col_bits = n_row.bit_length() - 1, n_col.bit_length() - 1
    assert n_row == 1 << row_bits and n_col == 1 << col_bits and row_bits >= 2 and col_bits >= 1
    col_low = 1
    core = n_col
    side = 2 * n_col
    others = [n_col << k for k in range(2, row_bits)] + [1 << k for k in range(1, col_bits)]
    my_row, my_col = lax.axis_index("row"), lax.axis_index("col")
    rank = (my_row * n_col + my_col).astype(jnp.int32)
    pivots = pivot_owner.shape[0]
    slots = 2 * pivots // devices + 2
    rows, width = features.shape
    depth = factor.shape[1]

    def pair(mask):
        return [(i, i ^ mask) for i in range(devices)]

    def staggered(mask_zero, mask_one):
        return [(i, i ^ (mask_one if i & core else mask_zero)) for i in range(devices)]

    first_pair = staggered(side, col_low)
    second_pair = staggered(col_low, side)

    def move(value, perm):
        return lax.ppermute(value, axes, perm)

    held = call(
        pick_kernel,
        jax.ShapeDtypeStruct((slots, width + 2 * depth), bf16),
        rank[None], pivot_owner[None, :], pivot_position[None, :], features, factor, smem=1,
    )
    for perm in [pair(mask) for mask in others] + [first_pair, second_pair]:
        held = jnp.concatenate([held, move(held, perm)], axis=0)
    far = move(held, pair(core))

    same_owner = pivot_owner[:, None] == pivot_owner[None, :]
    earlier = jnp.arange(pivots)[None, :] < jnp.arange(pivots)[:, None]
    slot_rank = jnp.sum((same_owner & earlier).astype(jnp.int32), axis=1)
    apart = pivot_owner ^ rank
    place = jnp.zeros_like(apart)
    bit = lambda mask: (apart & mask) // mask
    for k, mask in enumerate(others):
        place = place + bit(mask) * (1 << k)
    at = len(others)
    owner_core = (pivot_owner & core) // core
    low_bit = jnp.where(owner_core == 0, bit(side), bit(col_low))
    high_bit = jnp.where(owner_core == 0, bit(col_low), bit(side))
    place = place + low_bit * (1 << at) + high_bit * (2 << at) + bit(core) * (4 << at)
    source = (place * slots + slot_rank)[:, None]

    my_core = my_row & 1
    my_side = (my_row >> 1) & 1
    my_low = my_col & 1
    lead = jnp.where(my_core == 0, my_side, my_low)
    trail = jnp.where(my_core == 0, my_low, my_side)
    me = jnp.stack([my_core * 4 + lead * 2 + trail, (1 - my_core) * 4 + trail * 2 + lead]).astype(jnp.int32)
    weights = (ip_weights / (rows * devices))[:, None]
    total = depth + pivots
    piece = jax.ShapeDtypeStruct((4, pivots // 8, total), f32)
    residual, block, send, keep = call(
        residual_kernel,
        (
            jax.ShapeDtypeStruct((rows, pivots), f32),
            jax.ShapeDtypeStruct((pivots, pivots), f32),
            piece,
            piece,
        ),
        me, source, held, far, features, factor, weights, smem=1,
    )
    inverse = call(
        inverse_kernel,
        jax.ShapeDtypeStruct((pivots, pivots), f32),
        block,
        scratch=[pltpu.VMEM((pivots, pivots), f32)],
        flops=10**9,
    )
    keep = keep + move(send, pair(core))
    keep = keep[0:2] + move(keep[2:4], first_pair)
    keep = keep[0:1] + move(keep[1:2], second_pair)
    for mask in others:
        keep = keep + move(keep, pair(mask))
    keep = jnp.concatenate([keep, move(keep, second_pair)], axis=0)
    keep = jnp.concatenate([keep, move(keep, first_pair)], axis=0)
    other = move(keep, pair(core))
    new_columns = call(
        columns_kernel, jax.ShapeDtypeStruct((rows, pivots), f32), residual, inverse, flops=10**9
    )
    gram_rows = call(
        rows_kernel,
        jax.ShapeDtypeStruct((pivots, total), f32),
        me, keep, other, inverse,
        smem=1,
        scratch=[pltpu.VMEM((pivots, total), f32)],
    )
    return (new_columns, gram_rows)


def solution(mesh):
    placed = (P(("row", "col"), None), P(("row", "col"), None), P(("row", "col")), P(), P())
    return jax.shard_map(
        body, mesh=mesh, in_specs=placed, out_specs=(P(("row", "col"), None), P()), check_vma=False
    )
```

```python
import jax
import jax.numpy as jnp
from jax import lax
from jax.experimental import pallas as pl
from jax.experimental.pallas import tpu as pltpu
from jax.sharding import PartitionSpec as P

HIGHEST = lax.Precision.HIGHEST
f32 = jnp.float32
bf16 = jnp.bfloat16
i32 = jnp.int32
PANEL = 32


def dot(a, b, left, right, precision=None):
    return lax.dot_general(
        a, b, (((left,), (right,)), ((), ())), precision=precision, preferred_element_type=f32
    )


def nn(a, b, precision=None):
    return dot(a, b, 1, 0, precision)


def nt(a, b, precision=None):
    return dot(a, b, 1, 1, precision)


def tn(a, b, precision=None):
    return dot(a, b, 0, 0, precision)


def split(a):
    high = a.astype(bf16)
    low = (a - high.astype(f32)).astype(bf16)
    return high, low


def near(x):
    return pltpu.with_memory_space_constraint(x, pltpu.VMEM)


def call(kernel, outs, *args, smem=0, scratch=(), flops=10**9):
    specs = [pl.BlockSpec(memory_space=pltpu.SMEM)] * smem + [
        pl.BlockSpec(memory_space=pltpu.VMEM)
    ] * (len(args) - smem)
    return pl.pallas_call(
        kernel,
        out_shape=outs,
        in_specs=specs,
        out_specs=jax.tree.map(lambda _: pl.BlockSpec(memory_space=pltpu.VMEM), outs),
        scratch_shapes=scratch,
        compiler_params=pltpu.CompilerParams(vmem_limit_bytes=24 << 20),
        cost_estimate=pl.CostEstimate(flops=flops, transcendentals=0, bytes_accessed=10**6),
    )(*args)


def onehot(mask):
    return jnp.where(mask, 1.0, 0.0).astype(bf16)


def iota(shape, axis):
    return lax.broadcasted_iota(i32, shape, axis)


def pick_kernel(rank_ref, owner_ref, position_ref, features_ref, factor_ref, slots_ref):
    slots = slots_ref.shape[0]
    pivots = owner_ref.shape[1]
    rows, width = features_ref.shape
    depth = factor_ref.shape[1]
    mine = owner_ref[...] == rank_ref[0]
    ahead = onehot(iota((pivots, pivots), 0) < iota((pivots, pivots), 1))
    mine_rows = jnp.broadcast_to(jnp.where(mine, 1.0, 0.0), (8, pivots)).astype(bf16)
    order = nn(mine_rows, ahead)[0:1, :].astype(i32)
    chosen = onehot((iota((slots, pivots), 0) == order) & mine)
    located = onehot(iota((rows, pivots), 0) == position_ref[...])
    take = nt(chosen, located).astype(bf16)
    high, low = split(factor_ref[...])
    slots_ref[:, 0:width] = nn(take, features_ref[...]).astype(bf16)
    slots_ref[:, width : width + depth] = nn(take, high).astype(bf16)
    slots_ref[:, width + depth : width + 2 * depth] = nn(take, low).astype(bf16)


def prepare_kernel(core, side, col_low, others, slots, devices):
    def kernel(rank_ref, owner_ref, features_ref, factor_ref, source_ref, high_ref, low_ref, norm_ref):
        pivots = owner_ref.shape[1]
        owner = owner_ref[...]
        ahead = onehot(iota((pivots, pivots), 0) < iota((pivots, pivots), 1))
        owned = iota((devices, pivots), 0) == owner
        counts = nn(onehot(owned), ahead)
        slot_rank = jnp.sum(jnp.where(owned, counts, 0.0), axis=0, keepdims=True).astype(i32)
        apart = owner ^ rank_ref[0]
        bit = lambda mask: (apart >> (mask.bit_length() - 1)) & 1
        place = jnp.zeros_like(apart)
        for k, mask in enumerate(others):
            place = place + (bit(mask) << k)
        at = len(others)
        low_core = (owner & core) == 0
        lead = jnp.where(low_core, bit(side), bit(col_low))
        trail = jnp.where(low_core, bit(col_low), bit(side))
        place = place + (lead << at) + (trail << (at + 1)) + (bit(core) << (at + 2))
        source_ref[...] = place * slots + slot_rank
        high, low = split(factor_ref[...])
        high_ref[...] = high
        low_ref[...] = low
        wide = features_ref[...].astype(f32)
        norm_ref[...] = nt(jnp.ones((8, wide.shape[1]), f32), wide * wide, HIGHEST)[0:1, :]

    return kernel


def mixed(cross, left, right, width):
    base = jnp.exp((left + right - 2.0 * cross) * (-0.25 / width))
    square = base * base
    return 0.5 * base + 0.3 * square + 0.2 * (square * square)


def join_kernel(first_ref, second_ref, out_ref):
    n = first_ref.shape[0]
    out_ref[0:n, :] = first_ref[...]
    out_ref[n : 2 * n, :] = second_ref[...]


def gram_half(residual_ref, half, weights, high, low, order, out_ref):
    count, piece, _ = out_ref.shape
    size = count * piece
    depth = high.shape[1]
    rows = residual_ref[pl.ds(pl.multiple_of(half * size, size), size), :]
    weighted = rows * weights
    weighted_hi, weighted_lo = split(weighted)
    left = nn(weighted_hi, high) + (nn(weighted_lo, high) + nn(weighted_hi, low))
    right = nt(weighted, residual_ref[...], HIGHEST)
    for p in range(count):
        spot = (order & (count - 1)) ^ p
        out_ref[spot, :, 0:depth] = left[p * piece : (p + 1) * piece, :]
        out_ref[spot, :, depth:] = right[p * piece : (p + 1) * piece, :]


def residual_kernel(
    me_ref, source_ref, a_ref, b_ref, c_ref, d_ref, features_ref, high_ref, low_ref, norm_ref,
    weights_ref, pivot_ref, residual_ref, send_ref,
):
    pivots = source_ref.shape[1]
    held = a_ref.shape[0]
    width = features_ref.shape[1]
    depth = high_ref.shape[1]
    source = source_ref[...]
    place = iota((held, pivots), 0)
    pivot = None
    for k, ref in enumerate((a_ref, b_ref, c_ref, d_ref)):
        part = tn(onehot(place == source - k * held), ref[...])
        pivot = part if pivot is None else pivot + part
    pivot = pivot.astype(bf16)
    pivot_ref[...] = pivot
    pivot_x = pivot[:, 0:width]
    pivot_hi = pivot[:, width : width + depth]
    pivot_lo = pivot[:, width + depth :]
    high, low = high_ref[...], low_ref[...]
    pivot_wide = pivot_x.astype(f32)
    pivot_norm = jnp.sum(pivot_wide * pivot_wide, axis=1, keepdims=True)
    product = nt(pivot_hi, high) + (nt(pivot_lo, high) + nt(pivot_hi, low))
    residual_ref[...] = (
        mixed(nt(pivot_x, features_ref[...]), pivot_norm, norm_ref[...], width) - product
    )
    gram_half(residual_ref, 1 - me_ref[0], weights_ref[...], high, low, me_ref[2], send_ref)


def keep_kernel(me_ref, residual_ref, high_ref, low_ref, weights_ref, keep_ref):
    gram_half(
        residual_ref, me_ref[0], weights_ref[...], high_ref[...], low_ref[...], me_ref[1], keep_ref
    )


def eliminate(work_ref, k):
    n = work_ref.shape[0]
    size = PANEL
    lane = iota((size, n), 1)
    row_wide = iota((size, n), 0)
    row = iota((size, 128), 0)
    first = pl.multiple_of(k * size, size)
    rows = work_ref[pl.ds(first, size), :]
    slab = rows[:, 0:128]
    for g in range(1, n // 128):
        slab = jnp.where(first >= g * 128, rows[:, g * 128 : (g + 1) * 128], slab)
    slab = pltpu.roll(slab, (128 - first % 128) % 128, 1)
    columns = [jnp.broadcast_to(slab[:, j : j + 1], (size, 128)) for j in range(size)]
    scale = jnp.zeros((size, 128), f32)
    for j in range(size):
        pivot = columns[j][j : j + 1, :]
        scale = jnp.where(row == j, lax.rsqrt(pivot), scale)
        factor = jnp.where(row > j, columns[j] * (1.0 / pivot), 0.0)
        for l in range(j + 1, size):
            columns[l] = columns[l] - factor * columns[l][j : j + 1, :]
        rows = jnp.where(lane == first + j, jnp.where(row_wide == j, 1.0, 0.0), rows)
        rows = rows - jnp.concatenate([factor] * (n // 128), axis=1) * rows[j : j + 1, :]
    rows = rows * jnp.concatenate([scale] * (n // 128), axis=1)
    upper = jnp.where(lane >= first + size, rows, 0.0)
    update = tn(upper, rows, HIGHEST)
    full_lane, full_row = iota((n, n), 1), iota((n, n), 0)
    stale = (full_row >= first + size) & (full_lane >= first) & (full_lane < first + size)
    work_ref[...] = jnp.where(stale, 0.0, work_ref[...]) - update
    work_ref[pl.ds(first, size), :] = rows


def inverse_kernel(start, stop, width):
    def kernel(in_ref, work_ref):
        n = work_ref.shape[0]
        if start == 0:
            depth = (in_ref.shape[1] - width) // 2
            pivot_x = in_ref[:, 0:width]
            pivot_hi = in_ref[:, width : width + depth]
            pivot_lo = in_ref[:, width + depth :]
            wide = pivot_x.astype(f32)
            square = wide * wide
            left = jnp.sum(square, axis=1, keepdims=True)
            right = nt(jnp.ones((8, width), f32), square, HIGHEST)[0:1, :]
            product = nt(pivot_hi, pivot_hi) + (nt(pivot_lo, pivot_hi) + nt(pivot_hi, pivot_lo))
            work_ref[...] = mixed(nt(pivot_x, pivot_x), left, right, width) - product
        else:
            work_ref[...] = in_ref[...]

        def panel(k, carry):
            eliminate(work_ref, k)
            return carry

        lax.fori_loop(start, stop, panel, 0)
        if stop == n // PANEL:
            work_ref[...] = jnp.where(iota((n, n), 1) <= iota((n, n), 0), work_ref[...], 0.0)

    return kernel


def columns_kernel(residual_ref, inverse_ref, out_ref):
    out_ref[...] = dot(residual_ref[...], inverse_ref[...], 0, 1, HIGHEST)


def half_product(half, order, part_ref, inverse_ref, work_ref):
    count, piece, _ = part_ref.shape
    size = count * piece
    inverse = inverse_ref[...]
    picked = inverse[:, 0:size]
    for g in range(1, inverse.shape[1] // size):
        picked = jnp.where(half == g, inverse[:, g * size : (g + 1) * size], picked)
    for p in range(count):
        work_ref[p * piece : (p + 1) * piece, :] = part_ref[(order & (count - 1)) ^ p]
    return nn(picked, work_ref[...], HIGHEST)


def own_kernel(me_ref, part_ref, inverse_ref, out_ref, work_ref):
    out_ref[...] = half_product(me_ref[0], me_ref[1], part_ref, inverse_ref, work_ref)


def rows_kernel(me_ref, part_ref, inverse_ref, sum_ref, out_ref, work_ref):
    n = inverse_ref.shape[0]
    depth = out_ref.shape[1] - n
    out_ref[...] = half_product(1 - me_ref[0], me_ref[2], part_ref, inverse_ref, work_ref)
    total = sum_ref[...] + out_ref[...]
    out_ref[:, 0:depth] = total[:, 0:depth]
    out_ref[:, depth:] = nt(total[:, depth:], inverse_ref[...], HIGHEST)


def body(features, factor, ip_weights, pivot_owner, pivot_position):
    axes = ("row", "col")
    n_row, n_col = lax.axis_size("row"), lax.axis_size("col")
    devices = n_row * n_col
    row_bits, col_bits = n_row.bit_length() - 1, n_col.bit_length() - 1
    assert n_row == 1 << row_bits and n_col == 1 << col_bits and row_bits >= 2 and col_bits >= 1
    col_low = 1
    core = n_col
    side = 2 * n_col
    others = [n_col << k for k in range(2, row_bits)] + [1 << k for k in range(1, col_bits)]
    my_row, my_col = lax.axis_index("row"), lax.axis_index("col")
    rank = (my_row * n_col + my_col).astype(i32)[None]
    pivots = pivot_owner.shape[0]
    slots = 2 * pivots // devices + 2
    rows, width = features.shape
    depth = factor.shape[1]
    total = depth + pivots
    packed = width + 2 * depth

    def pair(mask):
        return [(i, i ^ mask) for i in range(devices)]

    def staggered(mask_zero, mask_one):
        return [(i, i ^ (mask_one if i & core else mask_zero)) for i in range(devices)]

    first_pair = staggered(side, col_low)
    second_pair = staggered(col_low, side)
    core_pair = pair(core)

    def move(value, perm):
        return lax.ppermute(value, axes, perm)

    owner_row = pivot_owner[None, :]
    held = call(
        pick_kernel,
        pltpu.VMEM((slots, packed), bf16),
        rank, owner_row, pivot_position[None, :], features, factor, smem=1,
    )
    for perm in [pair(mask) for mask in others] + [first_pair]:
        held = call(
            join_kernel, pltpu.VMEM((2 * held.shape[0], packed), bf16), held, near(move(held, perm))
        )
    source, high, low, norm = call(
        prepare_kernel(core, side, col_low, others, slots, devices),
        (
            pltpu.VMEM((1, pivots), i32),
            pltpu.VMEM((rows, depth), bf16),
            pltpu.VMEM((rows, depth), bf16),
            pltpu.VMEM((1, rows), f32),
        ),
        rank, owner_row, features, factor, smem=1,
    )
    across = near(move(held, second_pair))
    held_far = near(move(held, core_pair))
    across_far = near(move(across, core_pair))

    my_core = my_row & 1
    my_side = (my_row >> 1) & 1
    my_low = my_col & 1
    lead = jnp.where(my_core == 0, my_side, my_low)
    trail = jnp.where(my_core == 0, my_low, my_side)
    me = jnp.stack([my_core, lead * 2 + trail, trail * 2 + lead]).astype(i32)
    weights = (ip_weights / (rows * devices))[None, :]
    half = pltpu.VMEM((4, pivots // 8, total), f32)
    pivot, residual, send = call(
        residual_kernel,
        (pltpu.VMEM((pivots, packed), bf16), pltpu.VMEM((pivots, rows), f32), half),
        me, source, held, across, held_far, across_far, features, high, low, norm, weights, smem=1,
    )
    received = move(send, core_pair)
    keep = call(keep_kernel, half, me, residual, high, low, weights, smem=1)

    panels = pivots // PANEL
    windows = 4
    work = pivot

    def beside(value, perm, step):
        nonlocal work
        value, work = lax.optimization_barrier((value, work))
        got = move(value, perm)
        work = call(
            inverse_kernel(step * panels // windows, (step + 1) * panels // windows, width),
            pltpu.VMEM((pivots, pivots), f32),
            work,
        )
        got, work = lax.optimization_barrier((got, work))
        return got

    keep = keep + received
    keep = keep[0:2] + beside(keep[2:4], first_pair, 0)
    keep = keep[0:1] + beside(keep[1:2], second_pair, 1)
    step = 2
    for mask in others:
        if step < windows:
            keep = keep + beside(keep, pair(mask), step)
            step += 1
        else:
            keep = keep + move(keep, pair(mask))
    inverse = work
    new_columns = call(columns_kernel, jax.ShapeDtypeStruct((rows, pivots), f32), residual, inverse)
    keep = jnp.concatenate([keep, move(keep, second_pair)], axis=0)
    keep = near(jnp.concatenate([keep, move(keep, first_pair)], axis=0))
    other = near(move(keep, core_pair))
    scratch = [pltpu.VMEM((pivots // 2, total), f32)]
    own = call(
        own_kernel, pltpu.VMEM((pivots, total), f32), me, keep, inverse, smem=1, scratch=scratch
    )
    gram_rows = call(
        rows_kernel,
        jax.ShapeDtypeStruct((pivots, total), f32),
        me, other, inverse, own, smem=1, scratch=scratch,
    )
    return (new_columns, gram_rows)


def solution(mesh):
    placed = (P(("row", "col"), None), P(("row", "col"), None), P(("row", "col")), P(), P())
    return jax.shard_map(
        body, mesh=mesh, in_specs=placed, out_specs=(P(("row", "col"), None), P()), check_vma=False
    )
```

```python
from functools import partial

import jax
import jax.numpy as jnp
from jax import lax
from jax.experimental import pallas as pl
from jax.experimental.pallas import tpu as pltpu
from jax.sharding import PartitionSpec as P

HIGHEST = lax.Precision.HIGHEST
f32 = jnp.float32
bf16 = jnp.bfloat16
i32 = jnp.int32
PANEL = 32


def dot(a, b, left, right, precision=None):
    return lax.dot_general(
        a, b, (((left,), (right,)), ((), ())), precision=precision, preferred_element_type=f32
    )


def nn(a, b, precision=None):
    return dot(a, b, 1, 0, precision)


def nt(a, b, precision=None):
    return dot(a, b, 1, 1, precision)


def tn(a, b, precision=None):
    return dot(a, b, 0, 0, precision)


def split(a):
    high = a.astype(bf16)
    low = (a - high.astype(f32)).astype(bf16)
    return high, low


def near(x):
    return pltpu.with_memory_space_constraint(x, pltpu.VMEM)


def call(kernel, outs, *args, smem=0, scratch=(), flops=10**9):
    specs = [pl.BlockSpec(memory_space=pltpu.SMEM)] * smem + [
        pl.BlockSpec(memory_space=pltpu.VMEM)
    ] * (len(args) - smem)
    return pl.pallas_call(
        kernel,
        out_shape=outs,
        in_specs=specs,
        out_specs=jax.tree.map(lambda _: pl.BlockSpec(memory_space=pltpu.VMEM), outs),
        scratch_shapes=scratch,
        compiler_params=pltpu.CompilerParams(vmem_limit_bytes=24 << 20),
        cost_estimate=pl.CostEstimate(flops=flops, transcendentals=0, bytes_accessed=10**6),
    )(*args)


def onehot(mask):
    return jnp.where(mask, 1.0, 0.0).astype(bf16)


def iota(shape, axis):
    return lax.broadcasted_iota(i32, shape, axis)


def pick_kernel(chunks):
    def kernel(
        rank_ref, owner_ref, position_ref, features_ref, factor_ref,
        slots_ref, kept_ref, high_ref, low_ref,
        owner_in, position_in, factor_in, slots_sum, small_sems, factor_sems,
    ):
        slots = slots_ref.shape[0]
        pivots = owner_ref.shape[1]
        rows, width = features_ref.shape
        depth = factor_ref.shape[1]
        size = rows // chunks
        small = [
            pltpu.make_async_copy(source, target, small_sems.at[k])
            for k, (source, target) in enumerate(
                ((owner_ref, owner_in), (position_ref, position_in), (features_ref, kept_ref))
            )
        ]
        large = [
            pltpu.make_async_copy(
                factor_ref.at[pl.ds(k * size, size), :],
                factor_in.at[pl.ds(k * size, size), :],
                factor_sems.at[k],
            )
            for k in range(chunks)
        ]
        for copy in small + large:
            copy.start()
        ahead = onehot(iota((pivots, pivots), 0) < iota((pivots, pivots), 1))
        small[0].wait()
        mine = owner_in[...] == rank_ref[0]
        mine_rows = jnp.broadcast_to(jnp.where(mine, 1.0, 0.0), (8, pivots)).astype(bf16)
        order = nn(mine_rows, ahead)[0:1, :].astype(i32)
        chosen = onehot((iota((slots, pivots), 0) == order) & mine)
        small[1].wait()
        located = onehot(iota((rows, pivots), 0) == position_in[...])
        take = nt(chosen, located).astype(bf16)
        small[2].wait()
        slots_ref[:, 0:width] = nn(take, kept_ref[...]).astype(bf16)
        for k in range(chunks):
            large[k].wait()
            part = slice(k * size, (k + 1) * size)
            high, low = split(factor_in[part, :])
            high_ref[part, :] = high
            low_ref[part, :] = low
            for at, piece in ((0, high), (depth, low)):
                got = nn(take[:, part], piece)
                before = slots_sum[:, at : at + depth] if k else 0.0
                if k == chunks - 1:
                    slots_ref[:, width + at : width + at + depth] = (before + got).astype(bf16)
                else:
                    slots_sum[:, at : at + depth] = before + got

    return kernel


def prepare_kernel(core, side, col_low, others, slots, devices):
    def kernel(rank_ref, owner_ref, features_ref, source_ref, norm_ref):
        pivots = owner_ref.shape[1]
        owner = owner_ref[...]
        ahead = onehot(iota((pivots, pivots), 0) < iota((pivots, pivots), 1))
        owned = iota((devices, pivots), 0) == owner
        counts = nn(onehot(owned), ahead)
        slot_rank = jnp.sum(jnp.where(owned, counts, 0.0), axis=0, keepdims=True).astype(i32)
        apart = owner ^ rank_ref[0]
        bit = lambda mask: (apart >> (mask.bit_length() - 1)) & 1
        place = jnp.zeros_like(apart)
        for k, mask in enumerate(others):
            place = place + (bit(mask) << k)
        at = len(others)
        low_core = (owner & core) == 0
        lead = jnp.where(low_core, bit(side), bit(col_low))
        trail = jnp.where(low_core, bit(col_low), bit(side))
        place = place + (lead << at) + (trail << (at + 1)) + (bit(core) << (at + 2))
        source_ref[...] = place * slots + slot_rank
        wide = features_ref[...].astype(f32)
        norm_ref[...] = nt(jnp.ones((8, wide.shape[1]), f32), wide * wide, HIGHEST)[0:1, :]

    return kernel


def mixed(cross, left, right, width):
    base = jnp.exp((left + right - 2.0 * cross) * (-0.25 / width))
    square = base * base
    return 0.5 * base + 0.3 * square + 0.2 * (square * square)


def join_kernel(*refs):
    out_ref = refs[-1]
    at = 0
    for ref in refs[:-1]:
        out_ref[at : at + ref.shape[0]] = ref[...]
        at += ref.shape[0]


def spots(rank, core, side, col_low):
    bit = lambda mask: (rank >> (mask.bit_length() - 1)) & 1
    lead = jnp.where(bit(core) == 0, bit(side), bit(col_low))
    trail = jnp.where(bit(core) == 0, bit(col_low), bit(side))
    return bit(core), lead * 2 + trail, trail * 2 + lead


def gram_half(residual_ref, half, weights, high, low, order, out_ref):
    count, piece, _ = out_ref.shape
    size = count * piece
    depth = high.shape[1]
    rows = residual_ref[pl.ds(pl.multiple_of(half * size, size), size), :]
    weighted = rows * weights
    weighted_hi, weighted_lo = split(weighted)
    left = nn(weighted_hi, high) + (nn(weighted_lo, high) + nn(weighted_hi, low))
    right = nt(weighted, residual_ref[...], HIGHEST)
    for p in range(count):
        spot = (order & (count - 1)) ^ p
        out_ref[spot, :, 0:depth] = left[p * piece : (p + 1) * piece, :]
        out_ref[spot, :, depth:] = right[p * piece : (p + 1) * piece, :]


def residual_kernel(
    masks, samples, rank_ref, source_ref, a_ref, b_ref, c_ref, d_ref, features_ref, high_ref,
    low_ref, norm_ref, weights_ref, pivot_ref, residual_ref, send_ref,
):
    pivots = source_ref.shape[1]
    held = a_ref.shape[0]
    width = features_ref.shape[1]
    depth = high_ref.shape[1]
    source = source_ref[...]
    place = iota((held, pivots), 0)
    pivot = None
    for k, ref in enumerate((a_ref, b_ref, c_ref, d_ref)):
        part = tn(onehot(place == source - k * held), ref[...])
        pivot = part if pivot is None else pivot + part
    pivot = pivot.astype(bf16)
    pivot_ref[...] = pivot
    pivot_x = pivot[:, 0:width]
    pivot_hi = pivot[:, width : width + depth]
    pivot_lo = pivot[:, width + depth :]
    high, low = high_ref[...], low_ref[...]
    pivot_wide = pivot_x.astype(f32)
    pivot_norm = jnp.sum(pivot_wide * pivot_wide, axis=1, keepdims=True)
    product = nt(pivot_hi, high) + (nt(pivot_lo, high) + nt(pivot_hi, low))
    residual_ref[...] = (
        mixed(nt(pivot_x, features_ref[...]), pivot_norm, norm_ref[...], width) - product
    )
    core, _, order = spots(rank_ref[0], *masks)
    weights = weights_ref[...] / samples
    gram_half(residual_ref, 1 - core, weights, high, low, order, send_ref)


def keep_kernel(masks, samples, rank_ref, residual_ref, high_ref, low_ref, weights_ref, keep_ref):
    core, order, _ = spots(rank_ref[0], *masks)
    weights = weights_ref[...] / samples
    gram_half(residual_ref, core, weights, high_ref[...], low_ref[...], order, keep_ref)


def eliminate(work_ref, k):
    n = work_ref.shape[0]
    size = PANEL
    lane = iota((size, n), 1)
    row_wide = iota((size, n), 0)
    row = iota((size, 128), 0)
    first = pl.multiple_of(k * size, size)
    rows = work_ref[pl.ds(first, size), :]
    slab = rows[:, 0:128]
    for g in range(1, n // 128):
        slab = jnp.where(first >= g * 128, rows[:, g * 128 : (g + 1) * 128], slab)
    slab = pltpu.roll(slab, (128 - first % 128) % 128, 1)
    columns = [jnp.broadcast_to(slab[:, j : j + 1], (size, 128)) for j in range(size)]
    scale = jnp.zeros((size, 128), f32)
    for j in range(size):
        pivot = columns[j][j : j + 1, :]
        scale = jnp.where(row == j, lax.rsqrt(pivot), scale)
        factor = jnp.where(row > j, columns[j] * (1.0 / pivot), 0.0)
        for l in range(j + 1, size):
            columns[l] = columns[l] - factor * columns[l][j : j + 1, :]
        rows = jnp.where(lane == first + j, jnp.where(row_wide == j, 1.0, 0.0), rows)
        rows = rows - jnp.concatenate([factor] * (n // 128), axis=1) * rows[j : j + 1, :]
    rows = rows * jnp.concatenate([scale] * (n // 128), axis=1)
    upper = jnp.where(lane >= first + size, rows, 0.0)
    update = tn(upper, rows, HIGHEST)
    full_lane, full_row = iota((n, n), 1), iota((n, n), 0)
    stale = (full_row >= first + size) & (full_lane >= first) & (full_lane < first + size)
    work_ref[...] = jnp.where(stale, 0.0, work_ref[...]) - update
    work_ref[pl.ds(first, size), :] = rows


def inverse_kernel(start, stop, width):
    def kernel(in_ref, work_ref):
        n = work_ref.shape[0]
        if start == 0:
            depth = (in_ref.shape[1] - width) // 2
            pivot_x = in_ref[:, 0:width]
            pivot_hi = in_ref[:, width : width + depth]
            pivot_lo = in_ref[:, width + depth :]
            wide = pivot_x.astype(f32)
            square = wide * wide
            left = jnp.sum(square, axis=1, keepdims=True)
            right = nt(jnp.ones((8, width), f32), square, HIGHEST)[0:1, :]
            product = nt(pivot_hi, pivot_hi) + (nt(pivot_lo, pivot_hi) + nt(pivot_hi, pivot_lo))
            work_ref[...] = mixed(nt(pivot_x, pivot_x), left, right, width) - product
        else:
            work_ref[...] = in_ref[...]

        def panel(k, carry):
            eliminate(work_ref, k)
            return carry

        lax.fori_loop(start, stop, panel, 0)
        if stop == n // PANEL:
            work_ref[...] = jnp.where(iota((n, n), 1) <= iota((n, n), 0), work_ref[...], 0.0)

    return kernel


def columns_kernel(residual_ref, inverse_ref, out_ref):
    out_ref[...] = dot(residual_ref[...], inverse_ref[...], 0, 1, HIGHEST)


def half_product(half, order, part_ref, inverse_ref, work_ref):
    count, piece, _ = part_ref.shape
    size = count * piece
    inverse = inverse_ref[...]
    picked = inverse[:, 0:size]
    for g in range(1, inverse.shape[1] // size):
        picked = jnp.where(half == g, inverse[:, g * size : (g + 1) * size], picked)
    for p in range(count):
        work_ref[p * piece : (p + 1) * piece, :] = part_ref[(order & (count - 1)) ^ p]
    return nn(picked, work_ref[...], HIGHEST)


def own_kernel(masks, rank_ref, part_ref, inverse_ref, out_ref, work_ref):
    core, order, _ = spots(rank_ref[0], *masks)
    out_ref[...] = half_product(core, order, part_ref, inverse_ref, work_ref)


def rows_kernel(masks, rank_ref, part_ref, inverse_ref, sum_ref, out_ref, work_ref):
    n = inverse_ref.shape[0]
    depth = out_ref.shape[1] - n
    core, _, order = spots(rank_ref[0], *masks)
    out_ref[...] = half_product(1 - core, order, part_ref, inverse_ref, work_ref)
    total = sum_ref[...] + out_ref[...]
    out_ref[:, 0:depth] = total[:, 0:depth]
    out_ref[:, depth:] = nt(total[:, depth:], inverse_ref[...], HIGHEST)


def body(features, factor, ip_weights, pivot_owner, pivot_position):
    axes = ("row", "col")
    n_row, n_col = lax.axis_size("row"), lax.axis_size("col")
    devices = n_row * n_col
    row_bits, col_bits = n_row.bit_length() - 1, n_col.bit_length() - 1
    assert n_row == 1 << row_bits and n_col == 1 << col_bits and row_bits >= 2 and col_bits >= 1
    col_low = 1
    core = n_col
    side = 2 * n_col
    masks = (core, side, col_low)
    others = [n_col << k for k in range(2, row_bits)] + [1 << k for k in range(1, col_bits)]
    others = others[::-1]
    rank = (lax.axis_index("row") * n_col + lax.axis_index("col")).astype(i32)[None]
    pivots = pivot_owner.shape[0]
    slots = 2 * pivots // devices + 2
    rows, width = features.shape
    depth = factor.shape[1]
    samples = rows * devices
    total = depth + pivots
    packed = width + 2 * depth

    def pair(mask):
        return [(i, i ^ mask) for i in range(devices)]

    def staggered(mask_zero, mask_one):
        return [(i, i ^ (mask_one if i & core else mask_zero)) for i in range(devices)]

    first_pair = staggered(side, col_low)
    second_pair = staggered(col_low, side)
    both_pair = pair(side | col_low)
    core_pair = pair(core)

    def move(value, perm):
        return lax.ppermute(value, axes, perm)

    def tie(*values):
        return lax.optimization_barrier(values)

    owner_row = pivot_owner[None, :]
    chunks = 4
    far = lambda x: pltpu.with_memory_space_constraint(x, pltpu.HBM)
    held, kept, high, low = pl.pallas_call(
        pick_kernel(chunks),
        out_shape=(
            pltpu.VMEM((slots, packed), bf16),
            pltpu.VMEM((rows, width), bf16),
            pltpu.VMEM((rows, depth), bf16),
            pltpu.VMEM((rows, depth), bf16),
        ),
        in_specs=[pl.BlockSpec(memory_space=pltpu.SMEM)] + [pl.BlockSpec(memory_space=pltpu.HBM)] * 4,
        out_specs=tuple(pl.BlockSpec(memory_space=pltpu.VMEM) for _ in range(4)),
        scratch_shapes=[
            pltpu.VMEM((1, pivots), i32),
            pltpu.VMEM((1, pivots), i32),
            pltpu.VMEM((rows, depth), f32),
            pltpu.VMEM((slots, 2 * depth), f32),
            pltpu.SemaphoreType.DMA((3,)),
            pltpu.SemaphoreType.DMA((chunks,)),
        ],
        compiler_params=pltpu.CompilerParams(vmem_limit_bytes=24 << 20),
    )(rank, far(owner_row), far(pivot_position[None, :]), far(features), far(factor))
    prepared = None
    for perm in [pair(mask) for mask in others] + [first_pair]:
        got = near(move(held, perm))
        if prepared is None:
            source, norm = call(
                prepare_kernel(core, side, col_low, others, slots, devices),
                (pltpu.VMEM((1, pivots), i32), pltpu.VMEM((1, rows), f32)),
                rank, owner_row, kept, smem=1,
            )
            got, source, norm = tie(got, source, norm)
            prepared = True
        held = call(join_kernel, pltpu.VMEM((2 * held.shape[0], packed), bf16), held, got)
    across = near(move(held, second_pair))
    held_far = near(move(held, core_pair))
    across_far = near(move(across, core_pair))

    weights = ip_weights[None, :]
    half = pltpu.VMEM((4, pivots // 8, total), f32)
    pivot, residual, send = call(
        partial(residual_kernel, masks, samples),
        (pltpu.VMEM((pivots, packed), bf16), pltpu.VMEM((pivots, rows), f32), half),
        rank, source, held, across, held_far, across_far, kept, high, low, norm, weights, smem=1,
    )
    received = move(send, core_pair)
    keep = call(partial(keep_kernel, masks, samples), half, rank, residual, high, low, weights, smem=1)
    keep = keep + received

    panels = pivots // PANEL
    cuts = [0, panels // 4, panels * 5 // 8, panels]

    def eliminate_step(work, step):
        return call(
            inverse_kernel(cuts[step], cuts[step + 1], width), pltpu.VMEM((pivots, pivots), f32), work
        )

    keep, work = tie(keep, pivot)
    from_both = move(keep[3:4], both_pair)
    from_second = move(keep[1:2], second_pair)
    from_first = move(keep[2:3], first_pair)
    work = eliminate_step(work, 0)
    from_both, from_second, from_first, work = tie(from_both, from_second, from_first, work)
    keep = (keep[0:1] + from_both) + (from_second + from_first)
    step = 1
    for mask in others:
        got = move(keep, pair(mask))
        if step < len(cuts) - 1:
            work = eliminate_step(work, step)
            got, work = tie(got, work)
            step += 1
        keep = keep + got
    inverse = work
    keep, inverse = tie(keep, inverse)
    pieces = [keep] + [near(move(keep, perm)) for perm in (both_pair, second_pair, first_pair)]
    new_columns = call(columns_kernel, jax.ShapeDtypeStruct((rows, pivots), f32), residual, inverse)
    *pieces, new_columns = tie(*pieces, new_columns)
    keep = call(join_kernel, half, near(pieces[0]), pieces[2], pieces[3], pieces[1])
    other = near(move(keep, core_pair))
    scratch = [pltpu.VMEM((pivots // 2, total), f32)]
    own = call(
        partial(own_kernel, masks), pltpu.VMEM((pivots, total), f32), rank, keep, inverse,
        smem=1, scratch=scratch,
    )
    gram_rows = call(
        partial(rows_kernel, masks),
        jax.ShapeDtypeStruct((pivots, total), f32),
        rank, other, inverse, own, smem=1, scratch=scratch,
    )
    return (new_columns, gram_rows)


def solution(mesh):
    placed = (P(("row", "col"), None), P(("row", "col"), None), P(("row", "col")), P(), P())
    return jax.shard_map(
        body, mesh=mesh, in_specs=placed, out_specs=(P(("row", "col"), None), P()), check_vma=False
    )
```

```python
from functools import partial

import jax
import jax.numpy as jnp
from jax import lax
from jax.experimental import pallas as pl
from jax.experimental.pallas import tpu as pltpu
from jax.sharding import PartitionSpec as P

HIGHEST = lax.Precision.HIGHEST
f32 = jnp.float32
bf16 = jnp.bfloat16
i32 = jnp.int32
PANEL = 32
STEPS = 2.0**20


def dot(a, b, left, right, precision=None):
    return lax.dot_general(
        a, b, (((left,), (right,)), ((), ())), precision=precision, preferred_element_type=f32
    )


def nn(a, b, precision=None):
    return dot(a, b, 1, 0, precision)


def nt(a, b, precision=None):
    return dot(a, b, 1, 1, precision)


def tn(a, b, precision=None):
    return dot(a, b, 0, 0, precision)


def split(a):
    high = a.astype(bf16)
    low = (a - high.astype(f32)).astype(bf16)
    return high, low


def near(x):
    return pltpu.with_memory_space_constraint(x, pltpu.VMEM)


def call(kernel, outs, *args, smem=0, scratch=(), flops=10**9):
    specs = [pl.BlockSpec(memory_space=pltpu.SMEM)] * smem + [
        pl.BlockSpec(memory_space=pltpu.VMEM)
    ] * (len(args) - smem)
    return pl.pallas_call(
        kernel,
        out_shape=outs,
        in_specs=specs,
        out_specs=jax.tree.map(lambda _: pl.BlockSpec(memory_space=pltpu.VMEM), outs),
        scratch_shapes=scratch,
        compiler_params=pltpu.CompilerParams(vmem_limit_bytes=24 << 20),
        cost_estimate=pl.CostEstimate(flops=flops, transcendentals=0, bytes_accessed=10**6),
    )(*args)


def onehot(mask):
    return jnp.where(mask, 1.0, 0.0).astype(bf16)


def iota(shape, axis):
    return lax.broadcasted_iota(i32, shape, axis)


def pick_kernel(chunks):
    def kernel(
        rank_ref, owner_ref, position_ref, features_ref, factor_ref,
        slots_x_ref, slots_h_ref, kept_ref, high_ref, low_ref,
        owner_in, position_in, factor_in, slots_sum, small_sems, factor_sems,
    ):
        slots = slots_x_ref.shape[0]
        pivots = owner_ref.shape[1]
        rows, width = features_ref.shape
        depth = factor_ref.shape[1]
        size = rows // chunks
        small = [
            pltpu.make_async_copy(source, target, small_sems.at[k])
            for k, (source, target) in enumerate(
                ((owner_ref, owner_in), (position_ref, position_in), (features_ref, kept_ref))
            )
        ]
        large = [
            pltpu.make_async_copy(
                factor_ref.at[pl.ds(k * size, size), :],
                factor_in.at[pl.ds(k * size, size), :],
                factor_sems.at[k],
            )
            for k in range(chunks)
        ]
        for copy in small + large:
            copy.start()
        ahead = onehot(iota((pivots, pivots), 0) < iota((pivots, pivots), 1))
        small[0].wait()
        mine = owner_in[...] == rank_ref[0]
        mine_rows = jnp.broadcast_to(jnp.where(mine, 1.0, 0.0), (8, pivots)).astype(bf16)
        order = nn(mine_rows, ahead)[0:1, :].astype(i32)
        chosen = onehot((iota((slots, pivots), 0) == order) & mine)
        small[1].wait()
        located = onehot(iota((rows, pivots), 0) == position_in[...])
        take = nt(chosen, located).astype(bf16)
        small[2].wait()
        slots_x_ref[...] = nn(take, kept_ref[...]).astype(bf16)
        for k in range(chunks):
            large[k].wait()
            part = slice(k * size, (k + 1) * size)
            exact = factor_in[part, :]
            high, low = split(exact)
            high_ref[part, :] = high
            low_ref[part, :] = low
            rest = (exact - high.astype(f32) - low.astype(f32)).astype(bf16)
            chosen_rows = take[:, part]
            got = nn(chosen_rows, high) + (nn(chosen_rows, low) + nn(chosen_rows, rest))
            if k:
                got = slots_sum[...] + got
            if k < chunks - 1:
                slots_sum[...] = got
            else:
                slots_h_ref[...] = jnp.round(got * STEPS).astype(i32).astype(jnp.int16)

    return kernel


def prepare_kernel(core, side, col_low, others, slots, devices):
    def kernel(rank_ref, owner_ref, features_ref, source_ref, norm_ref):
        pivots = owner_ref.shape[1]
        owner = owner_ref[...]
        ahead = onehot(iota((pivots, pivots), 0) < iota((pivots, pivots), 1))
        owned = iota((devices, pivots), 0) == owner
        counts = nn(onehot(owned), ahead)
        slot_rank = jnp.sum(jnp.where(owned, counts, 0.0), axis=0, keepdims=True).astype(i32)
        apart = owner ^ rank_ref[0]
        bit = lambda mask: (apart >> (mask.bit_length() - 1)) & 1
        place = jnp.zeros_like(apart)
        for k, mask in enumerate(others):
            place = place + (bit(mask) << k)
        at = len(others)
        low_core = (owner & core) == 0
        lead = jnp.where(low_core, bit(side), bit(col_low))
        trail = jnp.where(low_core, bit(col_low), bit(side))
        place = place + (lead << at) + (trail << (at + 1)) + (bit(core) << (at + 2))
        source_ref[...] = place * slots + slot_rank
        wide = features_ref[...].astype(f32)
        norm_ref[...] = nt(jnp.ones((8, wide.shape[1]), f32), wide * wide, HIGHEST)[0:1, :]

    return kernel


def mixed(cross, left, right, width):
    base = jnp.exp((left + right - 2.0 * cross) * (-0.25 / width))
    square = base * base
    return 0.5 * base + 0.3 * square + 0.2 * (square * square)


def join_kernel(*refs):
    out_ref = refs[-1]
    at = 0
    for ref in refs[:-1]:
        out_ref[at : at + ref.shape[0]] = ref[...]
        at += ref.shape[0]


def spots(rank, core, side, col_low):
    bit = lambda mask: (rank >> (mask.bit_length() - 1)) & 1
    lead = jnp.where(bit(core) == 0, bit(side), bit(col_low))
    trail = jnp.where(bit(core) == 0, bit(col_low), bit(side))
    return bit(core), lead * 2 + trail, trail * 2 + lead


def gram_half(residual_ref, half, weights, high, low, order, out_ref):
    count, piece, _ = out_ref.shape
    size = count * piece
    depth = high.shape[1]
    rows = residual_ref[pl.ds(pl.multiple_of(half * size, size), size), :]
    weighted = rows * weights
    weighted_hi, weighted_lo = split(weighted)
    left = nn(weighted_hi, high) + (nn(weighted_lo, high) + nn(weighted_hi, low))
    right = nt(weighted, residual_ref[...], HIGHEST)
    for p in range(count):
        spot = (order & (count - 1)) ^ p
        out_ref[spot, :, 0:depth] = left[p * piece : (p + 1) * piece, :]
        out_ref[spot, :, depth:] = right[p * piece : (p + 1) * piece, :]


def ordered(source, start, x_ref, h_ref):
    held, width = x_ref.shape
    depth = h_ref.shape[1]
    chosen = onehot(iota((held, source.shape[1]), 0) == source - start)
    q = h_ref[...].astype(i32)
    coarse = (q + 128) >> 8
    fine = q - (coarse << 8)
    coarse = (coarse.astype(f32) * (256 / STEPS)).astype(bf16)
    fine = (fine.astype(f32) * (1 / STEPS)).astype(bf16)
    return [tn(chosen, part) for part in (x_ref[...], coarse, fine)]


def order_kernel(source_ref, a_x_ref, a_h_ref, c_x_ref, c_h_ref, pivot_ref):
    held, width = a_x_ref.shape
    depth = a_h_ref.shape[1]
    source = source_ref[...]
    near_parts = ordered(source, 0, a_x_ref, a_h_ref)
    far_parts = ordered(source, 2 * held, c_x_ref, c_h_ref)
    at = 0
    for one, two in zip(near_parts, far_parts):
        pivot_ref[:, at : at + one.shape[1]] = (one + two).astype(bf16)
        at += one.shape[1]


def residual_kernel(
    masks, samples, rank_ref, source_ref, partial_ref, b_x_ref, b_h_ref, d_x_ref, d_h_ref,
    features_ref, high_ref, low_ref, norm_ref, weights_ref, pivot_ref, residual_ref, send_ref,
):
    held, width = b_x_ref.shape
    depth = b_h_ref.shape[1]
    source = source_ref[...]
    across = ordered(source, held, b_x_ref, b_h_ref)
    beyond = ordered(source, 3 * held, d_x_ref, d_h_ref)
    pivot_x, pivot_hi, pivot_lo = [
        (one + two + partial_ref[:, at : at + one.shape[1]].astype(f32)).astype(bf16)
        for one, two, at in zip(across, beyond, (0, width, width + depth))
    ]
    pivot_ref[:, 0:width] = pivot_x
    pivot_ref[:, width : width + depth] = pivot_hi
    pivot_ref[:, width + depth :] = pivot_lo
    high, low = high_ref[...], low_ref[...]
    pivot_wide = pivot_x.astype(f32)
    pivot_norm = jnp.sum(pivot_wide * pivot_wide, axis=1, keepdims=True)
    product = nt(pivot_hi, high) + (nt(pivot_lo, high) + nt(pivot_hi, low))
    residual_ref[...] = (
        mixed(nt(pivot_x, features_ref[...]), pivot_norm, norm_ref[...], width) - product
    )
    core, _, order = spots(rank_ref[0], *masks)
    weights = weights_ref[...] / samples
    gram_half(residual_ref, 1 - core, weights, high, low, order, send_ref)


def keep_kernel(masks, samples, rank_ref, residual_ref, high_ref, low_ref, weights_ref, keep_ref):
    core, order, _ = spots(rank_ref[0], *masks)
    weights = weights_ref[...] / samples
    gram_half(residual_ref, core, weights, high_ref[...], low_ref[...], order, keep_ref)


def eliminate(work_ref, k):
    n = work_ref.shape[0]
    size = PANEL
    lane = iota((size, n), 1)
    row_wide = iota((size, n), 0)
    row = iota((size, 128), 0)
    first = pl.multiple_of(k * size, size)
    rows = work_ref[pl.ds(first, size), :]
    slab = rows[:, 0:128]
    for g in range(1, n // 128):
        slab = jnp.where(first >= g * 128, rows[:, g * 128 : (g + 1) * 128], slab)
    slab = pltpu.roll(slab, (128 - first % 128) % 128, 1)
    columns = [jnp.broadcast_to(slab[:, j : j + 1], (size, 128)) for j in range(size)]
    scale = jnp.zeros((size, 128), f32)
    for j in range(size):
        pivot = columns[j][j : j + 1, :]
        scale = jnp.where(row == j, lax.rsqrt(pivot), scale)
        factor = jnp.where(row > j, columns[j] * (1.0 / pivot), 0.0)
        for l in range(j + 1, size):
            columns[l] = columns[l] - factor * columns[l][j : j + 1, :]
        rows = jnp.where(lane == first + j, jnp.where(row_wide == j, 1.0, 0.0), rows)
        rows = rows - jnp.concatenate([factor] * (n // 128), axis=1) * rows[j : j + 1, :]
    rows = rows * jnp.concatenate([scale] * (n // 128), axis=1)
    upper = jnp.where(lane >= first + size, rows, 0.0)
    update = tn(upper, rows, HIGHEST)
    full_lane, full_row = iota((n, n), 1), iota((n, n), 0)
    stale = (full_row >= first + size) & (full_lane >= first) & (full_lane < first + size)
    work_ref[...] = jnp.where(stale, 0.0, work_ref[...]) - update
    work_ref[pl.ds(first, size), :] = rows


def inverse_kernel(start, stop, width):
    def kernel(in_ref, work_ref):
        n = work_ref.shape[0]
        if start == 0:
            depth = (in_ref.shape[1] - width) // 2
            pivot_x = in_ref[:, 0:width]
            pivot_hi = in_ref[:, width : width + depth]
            pivot_lo = in_ref[:, width + depth :]
            wide = pivot_x.astype(f32)
            square = wide * wide
            left = jnp.sum(square, axis=1, keepdims=True)
            right = nt(jnp.ones((8, width), f32), square, HIGHEST)[0:1, :]
            product = nt(pivot_hi, pivot_hi) + (nt(pivot_lo, pivot_hi) + nt(pivot_hi, pivot_lo))
            work_ref[...] = mixed(nt(pivot_x, pivot_x), left, right, width) - product
        else:
            work_ref[...] = in_ref[...]

        def panel(k, carry):
            eliminate(work_ref, k)
            return carry

        lax.fori_loop(start, stop, panel, 0)
        if stop == n // PANEL:
            work_ref[...] = jnp.where(iota((n, n), 1) <= iota((n, n), 0), work_ref[...], 0.0)

    return kernel


def columns_kernel(residual_ref, inverse_ref, out_ref):
    out_ref[...] = dot(residual_ref[...], inverse_ref[...], 0, 1, HIGHEST)


def half_product(half, order, part_ref, inverse_ref, work_ref):
    count, piece, _ = part_ref.shape
    size = count * piece
    inverse = inverse_ref[...]
    picked = inverse[:, 0:size]
    for g in range(1, inverse.shape[1] // size):
        picked = jnp.where(half == g, inverse[:, g * size : (g + 1) * size], picked)
    for p in range(count):
        work_ref[p * piece : (p + 1) * piece, :] = part_ref[(order & (count - 1)) ^ p]
    return nn(picked, work_ref[...], HIGHEST)


def own_kernel(masks, rank_ref, part_ref, inverse_ref, out_ref, work_ref):
    core, order, _ = spots(rank_ref[0], *masks)
    out_ref[...] = half_product(core, order, part_ref, inverse_ref, work_ref)


def rows_kernel(masks, rank_ref, part_ref, inverse_ref, sum_ref, out_ref, work_ref, done_ref, sems):
    n = inverse_ref.shape[0]
    depth = done_ref.shape[1] - n
    count, piece, total = part_ref.shape
    size = count * piece
    core, _, order = spots(rank_ref[0], *masks)
    inverse = inverse_ref[...]
    picked = inverse[:, 0:size]
    for g in range(1, n // size):
        picked = jnp.where(1 - core == g, inverse[:, g * size : (g + 1) * size], picked)
    for p in range(count):
        work_ref[p * piece : (p + 1) * piece, :] = part_ref[(order & (count - 1)) ^ p]
    cuts = [depth] + list(range(0, depth, depth // 2))
    for k, at in enumerate(cuts):
        here = slice(at, total if at == depth else at + depth // 2)
        done_ref[:, here] = nn(picked, work_ref[:, here], HIGHEST)
        done_ref[:, here] = sum_ref[:, here] + done_ref[:, here]
        if at == depth:
            done_ref[:, here] = nt(done_ref[:, here], inverse, HIGHEST)
        pltpu.make_async_copy(done_ref.at[:, here], out_ref.at[:, here], sems.at[k]).start()
    for k, at in enumerate(cuts):
        here = slice(at, total if at == depth else at + depth // 2)
        pltpu.make_async_copy(done_ref.at[:, here], out_ref.at[:, here], sems.at[k]).wait()


def body(features, factor, ip_weights, pivot_owner, pivot_position):
    axes = ("row", "col")
    n_row, n_col = lax.axis_size("row"), lax.axis_size("col")
    devices = n_row * n_col
    row_bits, col_bits = n_row.bit_length() - 1, n_col.bit_length() - 1
    assert n_row == 1 << row_bits and n_col == 1 << col_bits and row_bits >= 2 and col_bits >= 1
    col_low = 1
    core = n_col
    side = 2 * n_col
    masks = (core, side, col_low)
    others = [n_col << k for k in range(2, row_bits)] + [1 << k for k in range(1, col_bits)]
    others = others[::-1]
    rank = (lax.axis_index("row") * n_col + lax.axis_index("col")).astype(i32)[None]
    pivots = pivot_owner.shape[0]
    slots = 2 * pivots // devices + 2
    rows, width = features.shape
    depth = factor.shape[1]
    samples = rows * devices
    total = depth + pivots
    packed = width + 2 * depth

    def pair(mask):
        return [(i, i ^ mask) for i in range(devices)]

    def staggered(mask_zero, mask_one):
        return [(i, i ^ (mask_one if i & core else mask_zero)) for i in range(devices)]

    first_pair = staggered(side, col_low)
    second_pair = staggered(col_low, side)
    both_pair = pair(side | col_low)
    core_pair = pair(core)

    def move(value, perm):
        return lax.ppermute(value, axes, perm)

    def tie(*values):
        return lax.optimization_barrier(values)

    owner_row = pivot_owner[None, :]
    chunks = 4
    far = lambda x: pltpu.with_memory_space_constraint(x, pltpu.HBM)
    held_x, held_h, kept, high, low = pl.pallas_call(
        pick_kernel(chunks),
        out_shape=(
            pltpu.VMEM((slots, width), bf16),
            pltpu.VMEM((slots, depth), jnp.int16),
            pltpu.VMEM((rows, width), bf16),
            pltpu.VMEM((rows, depth), bf16),
            pltpu.VMEM((rows, depth), bf16),
        ),
        in_specs=[pl.BlockSpec(memory_space=pltpu.SMEM)] + [pl.BlockSpec(memory_space=pltpu.HBM)] * 4,
        out_specs=tuple(pl.BlockSpec(memory_space=pltpu.VMEM) for _ in range(5)),
        scratch_shapes=[
            pltpu.VMEM((1, pivots), i32),
            pltpu.VMEM((1, pivots), i32),
            pltpu.VMEM((rows, depth), f32),
            pltpu.VMEM((slots, depth), f32),
            pltpu.SemaphoreType.DMA((3,)),
            pltpu.SemaphoreType.DMA((chunks,)),
        ],
        compiler_params=pltpu.CompilerParams(vmem_limit_bytes=24 << 20),
    )(rank, far(owner_row), far(pivot_position[None, :]), far(features), far(factor))
    def joined(one, two):
        shape = (2 * one.shape[0], one.shape[1])
        return call(join_kernel, pltpu.VMEM(shape, one.dtype), one, two)

    prepared = False
    for perm in [pair(mask) for mask in others] + [first_pair]:
        got_h = near(move(held_h, perm))
        got_x = near(move(held_x, perm))
        if not prepared:
            source, norm = call(
                prepare_kernel(core, side, col_low, others, slots, devices),
                (pltpu.VMEM((1, pivots), i32), pltpu.VMEM((1, rows), f32)),
                rank, owner_row, kept, smem=1,
            )
            got_h, got_x, source, norm = tie(got_h, got_x, source, norm)
            prepared = True
        held_h, held_x = joined(held_h, got_h), joined(held_x, got_x)
    across_h, across_x = near(move(held_h, second_pair)), near(move(held_x, second_pair))
    far_h, far_x = near(move(held_h, core_pair)), near(move(held_x, core_pair))
    some = call(
        order_kernel, pltpu.VMEM((pivots, packed), bf16), source, held_x, held_h, far_x, far_h
    )
    across_h, across_x, some = tie(across_h, across_x, some)
    beyond_h, beyond_x = near(move(across_h, core_pair)), near(move(across_x, core_pair))

    weights = ip_weights[None, :]
    half = pltpu.VMEM((4, pivots // 8, total), f32)
    pivot, residual, send = call(
        partial(residual_kernel, masks, samples),
        (pltpu.VMEM((pivots, packed), bf16), pltpu.VMEM((pivots, rows), f32), half),
        rank, source, some, across_x, across_h, beyond_x, beyond_h, kept, high, low, norm, weights,
        smem=1,
    )
    received = move(send, core_pair)
    keep = call(partial(keep_kernel, masks, samples), half, rank, residual, high, low, weights, smem=1)
    keep = keep + received

    panels = pivots // PANEL
    cuts = [0, panels // 4, panels * 5 // 8, panels]

    def eliminate_step(work, step):
        return call(
            inverse_kernel(cuts[step], cuts[step + 1], width), pltpu.VMEM((pivots, pivots), f32), work
        )

    keep, work = tie(keep, pivot)
    from_both = move(keep[3:4], both_pair)
    from_second = move(keep[1:2], second_pair)
    from_first = move(keep[2:3], first_pair)
    work = eliminate_step(work, 0)
    from_both, from_second, from_first, work = tie(from_both, from_second, from_first, work)
    keep = (keep[0:1] + from_both) + (from_second + from_first)
    step = 1
    for mask in others:
        got = move(keep, pair(mask))
        if step < len(cuts) - 1:
            work = eliminate_step(work, step)
            got, work = tie(got, work)
            step += 1
        keep = keep + got
    inverse = work
    keep, inverse = tie(keep, inverse)
    pieces = [keep] + [near(move(keep, perm)) for perm in (both_pair, second_pair, first_pair)]
    new_columns = call(columns_kernel, jax.ShapeDtypeStruct((rows, pivots), f32), residual, inverse)
    *pieces, new_columns = tie(*pieces, new_columns)
    keep = call(join_kernel, half, near(pieces[0]), pieces[2], pieces[3], pieces[1])
    other = near(move(keep, core_pair))
    scratch = [pltpu.VMEM((pivots // 2, total), f32)]
    own = call(
        partial(own_kernel, masks), pltpu.VMEM((pivots, total), f32), rank, keep, inverse,
        smem=1, scratch=scratch,
    )
    gram_rows = pl.pallas_call(
        partial(rows_kernel, masks),
        out_shape=jax.ShapeDtypeStruct((pivots, total), f32),
        in_specs=[pl.BlockSpec(memory_space=pltpu.SMEM)] + [pl.BlockSpec(memory_space=pltpu.VMEM)] * 3,
        out_specs=pl.BlockSpec(memory_space=pltpu.HBM),
        scratch_shapes=[
            *scratch, pltpu.VMEM((pivots, total), f32), pltpu.SemaphoreType.DMA((3,))
        ],
        compiler_params=pltpu.CompilerParams(vmem_limit_bytes=24 << 20),
    )(rank, other, inverse, own)
    return (new_columns, gram_rows)


def solution(mesh):
    placed = (P(("row", "col"), None), P(("row", "col"), None), P(("row", "col")), P(), P())
    return jax.shard_map(
        body, mesh=mesh, in_specs=placed, out_specs=(P(("row", "col"), None), P()), check_vma=False
    )
```

```python
from functools import partial

import jax
import jax.numpy as jnp
from jax import lax
from jax.experimental import pallas as pl
from jax.experimental.pallas import tpu as pltpu
from jax.sharding import PartitionSpec as P


HIGHEST = lax.Precision.HIGHEST
f32 = jnp.float32
bf16 = jnp.bfloat16
i32 = jnp.int32
PANEL = 32
STEPS = 2.0**20


def dot(a, b, left, right, precision=None):
    return lax.dot_general(
        a, b, (((left,), (right,)), ((), ())), precision=precision, preferred_element_type=f32
    )


def nn(a, b, precision=None):
    return dot(a, b, 1, 0, precision)


def nt(a, b, precision=None):
    return dot(a, b, 1, 1, precision)


def tn(a, b, precision=None):
    return dot(a, b, 0, 0, precision)


def split(a):
    high = a.astype(bf16)
    low = (a - high.astype(f32)).astype(bf16)
    return high, low


def near(x):
    return pltpu.with_memory_space_constraint(x, pltpu.VMEM)


def call(kernel, outs, *args, smem=0, scratch=(), flops=10**9):
    specs = [pl.BlockSpec(memory_space=pltpu.SMEM)] * smem + [
        pl.BlockSpec(memory_space=pltpu.VMEM)
    ] * (len(args) - smem)
    return pl.pallas_call(
        kernel,
        out_shape=outs,
        in_specs=specs,
        out_specs=jax.tree.map(lambda _: pl.BlockSpec(memory_space=pltpu.VMEM), outs),
        scratch_shapes=scratch,
        compiler_params=pltpu.CompilerParams(vmem_limit_bytes=24 << 20),
        cost_estimate=pl.CostEstimate(flops=flops, transcendentals=0, bytes_accessed=10**6),
    )(*args)


def onehot(mask):
    return jnp.where(mask, 1.0, 0.0).astype(bf16)


def iota(shape, axis):
    return lax.broadcasted_iota(i32, shape, axis)


def pick_kernel(chunks):
    def kernel(
        rank_ref, owner_ref, position_ref, features_ref, factor_ref,
        slots_x_ref, slots_h_ref, kept_ref, high_ref, low_ref,
        owner_in, position_in, factor_in, slots_sum, small_sems, factor_sems,
    ):
        slots = slots_x_ref.shape[0]
        pivots = owner_ref.shape[1]
        rows, _ = features_ref.shape
        size = rows // chunks
        small = [
            pltpu.make_async_copy(source, target, small_sems.at[k])
            for k, (source, target) in enumerate(
                ((owner_ref, owner_in), (position_ref, position_in), (features_ref, kept_ref))
            )
        ]
        large = [
            pltpu.make_async_copy(
                factor_ref.at[pl.ds(k * size, size), :],
                factor_in.at[pl.ds(k * size, size), :],
                factor_sems.at[k],
            )
            for k in range(chunks)
        ]
        for copy in small + large:
            copy.start()
        ahead = onehot(iota((pivots, pivots), 0) < iota((pivots, pivots), 1))
        small[0].wait()
        mine = owner_in[...] == rank_ref[0]
        mine_rows = jnp.broadcast_to(jnp.where(mine, 1.0, 0.0), (8, pivots)).astype(bf16)
        order = nn(mine_rows, ahead)[0:1, :].astype(i32)
        chosen = onehot((iota((slots, pivots), 0) == order) & mine)
        small[1].wait()
        located = onehot(iota((rows, pivots), 0) == position_in[...])
        take = nt(chosen, located).astype(bf16)
        small[2].wait()
        slots_x_ref[...] = nn(take, kept_ref[...]).astype(bf16)
        for k in range(chunks):
            large[k].wait()
            part = slice(k * size, (k + 1) * size)
            exact = factor_in[part, :]
            high, low = split(exact)
            high_ref[part, :] = high
            low_ref[part, :] = low
            rest = (exact - high.astype(f32) - low.astype(f32)).astype(bf16)
            chosen_rows = take[:, part]
            got = nn(chosen_rows, high) + (nn(chosen_rows, low) + nn(chosen_rows, rest))
            if k:
                got = slots_sum[...] + got
            if k < chunks - 1:
                slots_sum[...] = got
            else:
                slots_h_ref[...] = jnp.round(got * STEPS).astype(i32).astype(jnp.int16)

    return kernel


def prepare_kernel(core, side, col_low, others, slots, devices):
    def kernel(rank_ref, owner_ref, features_ref, source_ref, norm_ref):
        pivots = owner_ref.shape[1]
        owner = owner_ref[...]
        ahead = onehot(iota((pivots, pivots), 0) < iota((pivots, pivots), 1))
        owned = iota((devices, pivots), 0) == owner
        counts = nn(onehot(owned), ahead)
        slot_rank = jnp.sum(jnp.where(owned, counts, 0.0), axis=0, keepdims=True).astype(i32)
        apart = owner ^ rank_ref[0]
        bit = lambda mask: (apart >> (mask.bit_length() - 1)) & 1
        place = jnp.zeros_like(apart)
        for k, mask in enumerate(others):
            place = place + (bit(mask) << k)
        at = len(others)
        low_core = (owner & core) == 0
        lead = jnp.where(low_core, bit(side), bit(col_low))
        trail = jnp.where(low_core, bit(col_low), bit(side))
        place = place + (lead << at) + (trail << (at + 1)) + (bit(core) << (at + 2))
        source_ref[...] = place * slots + slot_rank
        wide = features_ref[...].astype(f32)
        norm_ref[...] = nt(jnp.ones((8, wide.shape[1]), f32), wide * wide, HIGHEST)[0:1, :]

    return kernel


def mixed(cross, left, right, width):
    base = jnp.exp((left + right - 2.0 * cross) * (-0.25 / width))
    square = base * base
    return 0.5 * base + 0.3 * square + 0.2 * (square * square)


def join_kernel(*refs):
    out_ref = refs[-1]
    at = 0
    for ref in refs[:-1]:
        out_ref[at : at + ref.shape[0]] = ref[...]
        at += ref.shape[0]


def spots(rank, core, side, col_low):
    bit = lambda mask: (rank >> (mask.bit_length() - 1)) & 1
    lead = jnp.where(bit(core) == 0, bit(side), bit(col_low))
    trail = jnp.where(bit(core) == 0, bit(col_low), bit(side))
    return bit(core), lead * 2 + trail, trail * 2 + lead


def gram_half(residual_ref, half, weights, high, low, order, out_ref):
    count, piece, _ = out_ref.shape
    size = count * piece
    depth = high.shape[1]
    rows = residual_ref[pl.ds(pl.multiple_of(half * size, size), size), :]
    weighted = rows * weights
    weighted_hi, weighted_lo = split(weighted)
    left = nn(weighted_hi, high) + (nn(weighted_lo, high) + nn(weighted_hi, low))
    right = nt(weighted, residual_ref[...], HIGHEST)
    for p in range(count):
        spot = (order & (count - 1)) ^ p
        out_ref[spot, :, 0:depth] = left[p * piece : (p + 1) * piece, :]
        out_ref[spot, :, depth:] = right[p * piece : (p + 1) * piece, :]


def chosen_rows(source, start, held):
    return onehot(iota((held, source.shape[1]), 0) == source - start)


def ordered_h(source, start, h_ref):
    chosen = chosen_rows(source, start, h_ref.shape[0])
    q = h_ref[...].astype(i32)
    coarse = (q + 128) >> 8
    fine = q - (coarse << 8)
    coarse = (coarse.astype(f32) * (256 / STEPS)).astype(bf16)
    fine = (fine.astype(f32) * (1 / STEPS)).astype(bf16)
    return tn(chosen, coarse), tn(chosen, fine)


def ordered_x(source, start, x_ref):
    return tn(chosen_rows(source, start, x_ref.shape[0]), x_ref[...])


def order_kernel(source_ref, a_x_ref, a_h_ref, c_x_ref, c_h_ref, x_ref, coarse_ref, fine_ref):
    held = a_x_ref.shape[0]
    source = source_ref[...]
    x_ref[...] = (
        ordered_x(source, 0, a_x_ref) + ordered_x(source, 2 * held, c_x_ref)
    ).astype(bf16)
    one, two = ordered_h(source, 0, a_h_ref), ordered_h(source, 2 * held, c_h_ref)
    coarse_ref[...] = (one[0] + two[0]).astype(bf16)
    fine_ref[...] = (one[1] + two[1]).astype(bf16)


def across_kernel(source_ref, h_ref, coarse_in, fine_in, coarse_ref, fine_ref):
    coarse, fine = ordered_h(source_ref[...], h_ref.shape[0], h_ref)
    coarse_ref[...] = (coarse_in[...].astype(f32) + coarse).astype(bf16)
    fine_ref[...] = (fine_in[...].astype(f32) + fine).astype(bf16)


def product_kernel(
    source_ref, h_ref, coarse_in, fine_in, high_ref, low_ref, coarse_ref, fine_ref, product_ref
):
    coarse, fine = ordered_h(source_ref[...], 3 * h_ref.shape[0], h_ref)
    coarse = (coarse_in[...].astype(f32) + coarse).astype(bf16)
    fine = (fine_in[...].astype(f32) + fine).astype(bf16)
    coarse_ref[...] = coarse
    fine_ref[...] = fine
    high = high_ref[...]
    product_ref[...] = nt(coarse, high) + (nt(fine, high) + nt(coarse, low_ref[...]))


def residual_kernel(
    masks, samples, rank_ref, source_ref, x_ref, b_x_ref, d_x_ref, product_ref,
    features_ref, high_ref, low_ref, norm_ref, weights_ref, pivot_ref, residual_ref, send_ref,
):
    held, width = b_x_ref.shape
    source = source_ref[...]
    new = ordered_x(source, held, b_x_ref) + ordered_x(source, 3 * held, d_x_ref)
    pivot_x = (new + x_ref[...].astype(f32)).astype(bf16)
    pivot_ref[...] = pivot_x
    high, low = high_ref[...], low_ref[...]
    pivot_wide = pivot_x.astype(f32)
    pivot_norm = jnp.sum(pivot_wide * pivot_wide, axis=1, keepdims=True)
    residual_ref[...] = (
        mixed(nt(pivot_x, features_ref[...]), pivot_norm, norm_ref[...], width) - product_ref[...]
    )
    core, _, order = spots(rank_ref[0], *masks)
    weights = weights_ref[...] / samples
    gram_half(residual_ref, 1 - core, weights, high, low, order, send_ref)


def keep_kernel(masks, samples, rank_ref, residual_ref, high_ref, low_ref, weights_ref, keep_ref):
    core, order, _ = spots(rank_ref[0], *masks)
    weights = weights_ref[...] / samples
    gram_half(residual_ref, core, weights, high_ref[...], low_ref[...], order, keep_ref)


def eliminate(work_ref, k):
    n = work_ref.shape[0]
    size = PANEL
    lane = iota((size, n), 1)
    row_wide = iota((size, n), 0)
    row = iota((size, 128), 0)
    first = pl.multiple_of(k * size, size)
    rows = work_ref[pl.ds(first, size), :]
    slab = rows[:, 0:128]
    for g in range(1, n // 128):
        slab = jnp.where(first >= g * 128, rows[:, g * 128 : (g + 1) * 128], slab)
    slab = pltpu.roll(slab, (128 - first % 128) % 128, 1)
    columns = [jnp.broadcast_to(slab[:, j : j + 1], (size, 128)) for j in range(size)]
    scale = jnp.zeros((size, 128), f32)
    for j in range(size):
        pivot = columns[j][j : j + 1, :]
        scale = jnp.where(row == j, lax.rsqrt(pivot), scale)
        factor = jnp.where(row > j, columns[j] * (1.0 / pivot), 0.0)
        for l in range(j + 1, size):
            columns[l] = columns[l] - factor * columns[l][j : j + 1, :]
        rows = jnp.where(lane == first + j, jnp.where(row_wide == j, 1.0, 0.0), rows)
        rows = rows - jnp.concatenate([factor] * (n // 128), axis=1) * rows[j : j + 1, :]
    rows = rows * jnp.concatenate([scale] * (n // 128), axis=1)
    upper = jnp.where(lane >= first + size, rows, 0.0)
    update = tn(upper, rows, HIGHEST)
    full_lane, full_row = iota((n, n), 1), iota((n, n), 0)
    stale = (full_row >= first + size) & (full_lane >= first) & (full_lane < first + size)
    work_ref[...] = jnp.where(stale, 0.0, work_ref[...]) - update
    work_ref[pl.ds(first, size), :] = rows


def inverse_kernel(start, stop):
    def kernel(*refs):
        work_ref = refs[-1]
        n = work_ref.shape[0]
        if start == 0:
            pivot_x, pivot_hi, pivot_lo = [ref[...] for ref in refs[:3]]
            width = pivot_x.shape[1]
            wide = pivot_x.astype(f32)
            square = wide * wide
            left = jnp.sum(square, axis=1, keepdims=True)
            right = nt(jnp.ones((8, width), f32), square, HIGHEST)[0:1, :]
            product = nt(pivot_hi, pivot_hi) + (nt(pivot_lo, pivot_hi) + nt(pivot_hi, pivot_lo))
            work_ref[...] = mixed(nt(pivot_x, pivot_x), left, right, width) - product
        else:
            work_ref[...] = refs[0][...]

        def panel(k, carry):
            eliminate(work_ref, k)
            return carry

        lax.fori_loop(start, stop, panel, 0)
        if stop == n // PANEL:
            work_ref[...] = jnp.where(iota((n, n), 1) <= iota((n, n), 0), work_ref[...], 0.0)

    return kernel


def columns_kernel(residual_ref, inverse_ref, out_ref):
    out_ref[...] = dot(residual_ref[...], inverse_ref[...], 0, 1, HIGHEST)


def rows_kernel(masks, rank_ref, *refs):
    inverse_ref, out_ref, work_ref, done_ref, sems = refs[-5:]
    parts = refs[:-5]
    count = len(parts) // 2
    piece = parts[0].shape[1]
    n = inverse_ref.shape[0]
    total = done_ref.shape[1]
    depth = total - n
    core, near_order, far_order = spots(rank_ref[0], *masks)
    for k, part in enumerate(parts):
        mine = k < count
        half = core if mine else 1 - core
        at = half * count + ((near_order if mine else far_order) ^ (k % count))
        work_ref[pl.ds(pl.multiple_of(at * piece, piece), piece), :] = part[0]
    inverse = inverse_ref[...]
    copies = []
    for k, at in enumerate([depth] + list(range(0, depth, depth // 2))):
        here = slice(at, total if at == depth else at + depth // 2)
        done = nn(inverse, work_ref[:, here], HIGHEST)
        if at == depth:
            done = nt(done, inverse, HIGHEST)
        done_ref[:, here] = done
        copies.append(pltpu.make_async_copy(done_ref.at[:, here], out_ref.at[:, here], sems.at[k]))
        copies[-1].start()
    for copy in copies:
        copy.wait()


def body(features, factor, ip_weights, pivot_owner, pivot_position):
    axes = ("row", "col")
    n_row, n_col = lax.axis_size("row"), lax.axis_size("col")
    devices = n_row * n_col
    row_bits, col_bits = n_row.bit_length() - 1, n_col.bit_length() - 1
    assert n_row == 1 << row_bits and n_col == 1 << col_bits and row_bits >= 2 and col_bits >= 1
    col_low = 1
    core = n_col
    side = 2 * n_col
    masks = (core, side, col_low)
    others = [n_col << k for k in range(2, row_bits)] + [1 << k for k in range(1, col_bits)]
    others = others[::-1]
    rank = (lax.axis_index("row") * n_col + lax.axis_index("col")).astype(i32)[None]
    pivots = pivot_owner.shape[0]
    slots = 2 * pivots // devices + 2
    rows, width = features.shape
    depth = factor.shape[1]
    samples = rows * devices
    total = depth + pivots

    def pair(mask):
        return [(i, i ^ mask) for i in range(devices)]

    def staggered(mask_zero, mask_one):
        return [(i, i ^ (mask_one if i & core else mask_zero)) for i in range(devices)]

    first_pair = staggered(side, col_low)
    second_pair = staggered(col_low, side)
    both_pair = pair(side | col_low)
    core_pair = pair(core)

    def move(value, perm):
        return lax.ppermute(value, axes, perm)

    def tie(*values):
        return lax.optimization_barrier(values)

    owner_row = pivot_owner[None, :]
    chunks = 4
    far = lambda x: pltpu.with_memory_space_constraint(x, pltpu.HBM)
    held_x, held_h, kept, high, low = pl.pallas_call(
        pick_kernel(chunks),
        out_shape=(
            pltpu.VMEM((slots, width), bf16),
            pltpu.VMEM((slots, depth), jnp.int16),
            pltpu.VMEM((rows, width), bf16),
            pltpu.VMEM((rows, depth), bf16),
            pltpu.VMEM((rows, depth), bf16),
        ),
        in_specs=[pl.BlockSpec(memory_space=pltpu.SMEM)] + [pl.BlockSpec(memory_space=pltpu.HBM)] * 4,
        out_specs=tuple(pl.BlockSpec(memory_space=pltpu.VMEM) for _ in range(5)),
        scratch_shapes=[
            pltpu.VMEM((1, pivots), i32),
            pltpu.VMEM((1, pivots), i32),
            pltpu.VMEM((rows, depth), f32),
            pltpu.VMEM((slots, depth), f32),
            pltpu.SemaphoreType.DMA((3,)),
            pltpu.SemaphoreType.DMA((chunks,)),
        ],
        compiler_params=pltpu.CompilerParams(vmem_limit_bytes=24 << 20),
    )(rank, far(owner_row), far(pivot_position[None, :]), far(features), far(factor))

    def joined(one, two):
        shape = (2 * one.shape[0], one.shape[1])
        return call(join_kernel, pltpu.VMEM(shape, one.dtype), one, two)

    prepared = False
    perms = [pair(mask) for mask in others] + [first_pair]
    for perm in perms:
        got_h = near(move(held_h, perm))
        got_x = near(move(held_x, perm))
        if not prepared:
            source, norm = call(
                prepare_kernel(core, side, col_low, others, slots, devices),
                (pltpu.VMEM((1, pivots), i32), pltpu.VMEM((1, rows), f32)),
                rank, owner_row, kept, smem=1,
            )
            got_h, got_x, source, norm = tie(got_h, got_x, source, norm)
            prepared = True
        held_h = joined(held_h, got_h)
        held_x = joined(held_x, got_x)
    across_h = near(move(held_h, second_pair))
    across_x = near(move(held_x, second_pair))
    far_h, far_x = near(move(held_h, core_pair)), near(move(held_x, core_pair))
    plane = pltpu.VMEM((pivots, depth), bf16)
    pivot_x, coarse, fine = call(
        order_kernel,
        (pltpu.VMEM((pivots, width), bf16), plane, plane),
        source, held_x, held_h, far_x, far_h,
    )
    across_h, coarse, fine = tie(across_h, coarse, fine)
    beyond_h = near(move(across_h, core_pair))
    coarse, fine = call(across_kernel, (plane, plane), source, across_h, coarse, fine)
    across_x, coarse, fine = tie(across_x, coarse, fine)
    beyond_x = near(move(across_x, core_pair))
    coarse, fine, product = call(
        product_kernel,
        (plane, plane, pltpu.VMEM((pivots, rows), f32)),
        source, beyond_h, coarse, fine, high, low,
    )
    beyond_x, product = tie(beyond_x, product)

    weights = ip_weights[None, :]
    half = pltpu.VMEM((4, pivots // 8, total), f32)
    pivot_x, residual, send = call(
        partial(residual_kernel, masks, samples),
        (pltpu.VMEM((pivots, width), bf16), pltpu.VMEM((pivots, rows), f32), half),
        rank, source, pivot_x, across_x, beyond_x, product, kept, high, low, norm, weights,
        smem=1,
    )
    received = move(send, core_pair)
    keep = call(partial(keep_kernel, masks, samples), half, rank, residual, high, low, weights, smem=1)
    keep = keep + received

    panels = pivots // PANEL
    cuts = [0, panels // 4, panels * 5 // 8, panels]

    def eliminate_step(step, *given):
        return call(
            inverse_kernel(cuts[step], cuts[step + 1]), pltpu.VMEM((pivots, pivots), f32), *given
        )

    keep, pivot_x, coarse, fine = tie(keep, pivot_x, coarse, fine)
    from_both = move(keep[3:4], both_pair)
    from_second = move(keep[1:2], second_pair)
    from_first = move(keep[2:3], first_pair)
    work = eliminate_step(0, pivot_x, coarse, fine)
    from_both, from_second, from_first, work = tie(from_both, from_second, from_first, work)
    keep = (keep[0:1] + from_both) + (from_second + from_first)
    step = 1
    for mask in others:
        got = move(keep, pair(mask))
        if step < len(cuts) - 1:
            work = eliminate_step(step, work)
            got, work = tie(got, work)
            step += 1
        keep = keep + got
    inverse = work
    keep, inverse = tie(keep, inverse)
    pieces = [near(keep)] + [near(move(keep, perm)) for perm in (second_pair, first_pair, both_pair)]
    new_columns = call(columns_kernel, jax.ShapeDtypeStruct((rows, pivots), f32), residual, inverse)
    pieces[3], new_columns = tie(pieces[3], new_columns)
    pieces += [near(move(piece, core_pair)) for piece in pieces]
    gram_rows = pl.pallas_call(
        partial(rows_kernel, masks),
        out_shape=jax.ShapeDtypeStruct((pivots, total), f32),
        in_specs=[pl.BlockSpec(memory_space=pltpu.SMEM)] + [pl.BlockSpec(memory_space=pltpu.VMEM)] * 9,
        out_specs=pl.BlockSpec(memory_space=pltpu.HBM),
        scratch_shapes=[
            pltpu.VMEM((pivots, total), f32),
            pltpu.VMEM((pivots, total), f32),
            pltpu.SemaphoreType.DMA((3,)),
        ],
        compiler_params=pltpu.CompilerParams(vmem_limit_bytes=24 << 20),
    )(rank, *pieces, inverse)
    return (new_columns, gram_rows)


def solution(mesh):
    placed = (P(("row", "col"), None), P(("row", "col"), None), P(("row", "col")), P(), P())

    return jax.shard_map(
        body, mesh=mesh, in_specs=placed, out_specs=(P(("row", "col"), None), P()), check_vma=False
    )
```

```python
from functools import partial

import jax
import jax.numpy as jnp
from jax import lax
from jax.experimental import pallas as pl
from jax.experimental.pallas import tpu as pltpu
from jax.sharding import PartitionSpec as P


HIGHEST = lax.Precision.HIGHEST
f32 = jnp.float32
bf16 = jnp.bfloat16
i32 = jnp.int32
PANEL = 32
STEPS = 2.0**20


def dot(a, b, left, right, precision=None):
    return lax.dot_general(
        a, b, (((left,), (right,)), ((), ())), precision=precision, preferred_element_type=f32
    )


def nn(a, b, precision=None):
    return dot(a, b, 1, 0, precision)


def nt(a, b, precision=None):
    return dot(a, b, 1, 1, precision)


def tn(a, b, precision=None):
    return dot(a, b, 0, 0, precision)


def split(a):
    high = a.astype(bf16)
    low = (a - high.astype(f32)).astype(bf16)
    return high, low


def near(x):
    return pltpu.with_memory_space_constraint(x, pltpu.VMEM)


def call(kernel, outs, *args, smem=0, scratch=(), flops=10**9):
    specs = [pl.BlockSpec(memory_space=pltpu.SMEM)] * smem + [
        pl.BlockSpec(memory_space=pltpu.VMEM)
    ] * (len(args) - smem)
    return pl.pallas_call(
        kernel,
        out_shape=outs,
        in_specs=specs,
        out_specs=jax.tree.map(lambda _: pl.BlockSpec(memory_space=pltpu.VMEM), outs),
        scratch_shapes=scratch,
        compiler_params=pltpu.CompilerParams(vmem_limit_bytes=24 << 20),
        cost_estimate=pl.CostEstimate(flops=flops, transcendentals=0, bytes_accessed=10**6),
    )(*args)


def onehot(mask):
    return jnp.where(mask, 1.0, 0.0).astype(bf16)


def iota(shape, axis):
    return lax.broadcasted_iota(i32, shape, axis)


def pick_kernel(
    rank_ref, owner_ref, position_ref, features_ref, factor_ref,
    slots_x_ref, slots_h_ref, kept_ref, factor_in,
    owner_in, position_in, owner_list, position_list, found, rows_in, sems,
):
    slots = slots_x_ref.shape[0]
    pivots = owner_ref.shape[1]
    rows = features_ref.shape[0]
    half = rows // 2
    pairs = [
        (owner_ref, owner_list),
        (position_ref, position_list),
        (owner_ref, owner_in),
        (position_ref, position_in),
        (features_ref, kept_ref),
        (factor_ref.at[pl.ds(0, half), :], factor_in.at[pl.ds(0, half), :]),
        (factor_ref.at[pl.ds(half, half), :], factor_in.at[pl.ds(half, half), :]),
    ]
    copies = [
        pltpu.make_async_copy(source, target, sems.at[k]) for k, (source, target) in enumerate(pairs)
    ]
    for copy in copies:
        copy.start()
    rank = rank_ref[0]
    for k in range(slots + 1):
        found[k] = 0
    copies[0].wait()
    copies[1].wait()

    def collect(k, count):
        for p in range(8):
            at = k * 8 + p
            found[count] = position_list[0, at]
            count = jnp.minimum(count + (owner_list[0, at] == rank).astype(i32), slots)
        return count

    lax.fori_loop(0, pivots // 8, collect, jnp.int32(0))
    ahead = onehot(iota((pivots, pivots), 0) < iota((pivots, pivots), 1))
    copies[2].wait()
    mine = owner_in[...] == rank
    mine_rows = jnp.broadcast_to(jnp.where(mine, 1.0, 0.0), (8, pivots)).astype(bf16)
    order = nn(mine_rows, ahead)[0:1, :].astype(i32)
    chosen = onehot((iota((slots, pivots), 0) == order) & mine)
    copies[3].wait()
    located = onehot(iota((rows, pivots), 0) == position_in[...])
    take = nt(chosen, located).astype(bf16)
    copies[4].wait()
    slots_x_ref[...] = nn(take, kept_ref[...]).astype(bf16)
    copies[5].wait()
    copies[6].wait()
    for k in range(slots):
        rows_in[k : k + 1, :] = factor_in[pl.ds(found[k], 1), :]
    slots_h_ref[...] = jnp.round(rows_in[...] * STEPS).astype(i32).astype(jnp.int16)


def prepare_kernel(core, side, col_low, others, slots, devices):
    def kernel(
        rank_ref, owner_ref, features_ref, factor_ref, source_ref, norm_ref, high_ref, low_ref
    ):
        pivots = owner_ref.shape[1]
        owner = owner_ref[...]
        ahead = onehot(iota((pivots, pivots), 0) < iota((pivots, pivots), 1))
        owned = iota((devices, pivots), 0) == owner
        counts = nn(onehot(owned), ahead)
        slot_rank = jnp.sum(jnp.where(owned, counts, 0.0), axis=0, keepdims=True).astype(i32)
        apart = owner ^ rank_ref[0]
        bit = lambda mask: (apart >> (mask.bit_length() - 1)) & 1
        place = jnp.zeros_like(apart)
        for k, mask in enumerate(others):
            place = place + (bit(mask) << k)
        at = len(others)
        low_core = (owner & core) == 0
        lead = jnp.where(low_core, bit(side), bit(col_low))
        trail = jnp.where(low_core, bit(col_low), bit(side))
        place = place + (lead << at) + (trail << (at + 1)) + (bit(core) << (at + 2))
        source_ref[...] = place * slots + slot_rank
        high, low = split(factor_ref[...])
        high_ref[...] = high
        low_ref[...] = low
        wide = features_ref[...].astype(f32)
        norm_ref[...] = nt(jnp.ones((8, wide.shape[1]), f32), wide * wide, HIGHEST)[0:1, :]

    return kernel


def mixed(cross, left, right, width):
    base = jnp.exp((left + right - 2.0 * cross) * (-0.25 / width))
    square = base * base
    return 0.5 * base + 0.3 * square + 0.2 * (square * square)


def join_kernel(*refs):
    out_ref = refs[-1]
    at = 0
    for ref in refs[:-1]:
        out_ref[at : at + ref.shape[0]] = ref[...]
        at += ref.shape[0]


def spots(rank, core, side, col_low):
    bit = lambda mask: (rank >> (mask.bit_length() - 1)) & 1
    lead = jnp.where(bit(core) == 0, bit(side), bit(col_low))
    trail = jnp.where(bit(core) == 0, bit(col_low), bit(side))
    return bit(core), lead * 2 + trail, trail * 2 + lead


def gram_half(residual_ref, half, weights, high, low, order, out_ref):
    count, piece, _ = out_ref.shape
    size = count * piece
    depth = high.shape[1]
    n = residual_ref.shape[0]
    upper = residual_ref[pl.ds(pl.multiple_of(half * size, size), size), :]
    lower = residual_ref[pl.ds(pl.multiple_of(n // 2 + half * size, size), size), :]
    weighted = jnp.concatenate([upper, lower], axis=0) * weights
    weighted_hi, weighted_lo = split(weighted)
    left = nn(weighted_hi, high) + (nn(weighted_lo, high) + nn(weighted_hi, low))
    residual = residual_ref[...]
    top = nt(weighted[0:size], residual, HIGHEST)
    bottom = nt(weighted[size:], residual[n // 2 :], HIGHEST)
    for p in range(count):
        spot = (order & (count - 1)) ^ p
        rows = slice(p * piece, (p + 1) * piece)
        out_ref[spot, :, 0:depth] = left[rows]
        out_ref[spot, :, depth : 2 * depth] = left[size + p * piece : size + (p + 1) * piece]
        out_ref[spot, :, 2 * depth : 2 * depth + n] = top[rows]
        out_ref[spot, :, 2 * depth + n :] = bottom[rows]


def chosen_rows(source, start, held):
    return onehot(iota((held, source.shape[1]), 0) == source - start)


def ordered_h(source, start, h_ref):
    chosen = chosen_rows(source, start, h_ref.shape[0])
    q = h_ref[...].astype(i32)
    coarse = (q + 128) >> 8
    fine = q - (coarse << 8)
    coarse = (coarse.astype(f32) * (256 / STEPS)).astype(bf16)
    fine = (fine.astype(f32) * (1 / STEPS)).astype(bf16)
    return tn(chosen, coarse), tn(chosen, fine)


def ordered_x(source, start, x_ref):
    return tn(chosen_rows(source, start, x_ref.shape[0]), x_ref[...])


def order_kernel(source_ref, a_x_ref, a_h_ref, c_x_ref, c_h_ref, x_ref, coarse_ref, fine_ref):
    held = a_x_ref.shape[0]
    source = source_ref[...]
    x_ref[...] = (
        ordered_x(source, 0, a_x_ref) + ordered_x(source, 2 * held, c_x_ref)
    ).astype(bf16)
    one, two = ordered_h(source, 0, a_h_ref), ordered_h(source, 2 * held, c_h_ref)
    coarse_ref[...] = (one[0] + two[0]).astype(bf16)
    fine_ref[...] = (one[1] + two[1]).astype(bf16)


def across_kernel(place, source_ref, h_ref, coarse_in, fine_in, coarse_ref, fine_ref):
    coarse, fine = ordered_h(source_ref[...], place * h_ref.shape[0], h_ref)
    coarse_ref[...] = (coarse_in[...].astype(f32) + coarse).astype(bf16)
    fine_ref[...] = (fine_in[...].astype(f32) + fine).astype(bf16)


def product_kernel(coarse_ref, fine_ref, high_ref, low_ref, product_ref):
    coarse, high = coarse_ref[...], high_ref[...]
    product_ref[...] = nt(coarse, high) + (nt(fine_ref[...], high) + nt(coarse, low_ref[...]))


def residual_kernel(
    masks, samples, rank_ref, source_ref, x_ref, b_x_ref, d_x_ref, product_ref,
    features_ref, high_ref, low_ref, norm_ref, weights_ref, pivot_ref, residual_ref, send_ref,
):
    held, width = b_x_ref.shape
    source = source_ref[...]
    new = ordered_x(source, held, b_x_ref) + ordered_x(source, 3 * held, d_x_ref)
    pivot_x = (new + x_ref[...].astype(f32)).astype(bf16)
    pivot_ref[...] = pivot_x
    high, low = high_ref[...], low_ref[...]
    pivot_wide = pivot_x.astype(f32)
    pivot_norm = jnp.sum(pivot_wide * pivot_wide, axis=1, keepdims=True)
    residual_ref[...] = (
        mixed(nt(pivot_x, features_ref[...]), pivot_norm, norm_ref[...], width) - product_ref[...]
    )
    core, _, order = spots(rank_ref[0], *masks)
    weights = weights_ref[...] / samples
    gram_half(residual_ref, 1 - core, weights, high, low, order, send_ref)


def keep_kernel(masks, samples, rank_ref, residual_ref, high_ref, low_ref, weights_ref, keep_ref):
    core, order, _ = spots(rank_ref[0], *masks)
    weights = weights_ref[...] / samples
    gram_half(residual_ref, core, weights, high_ref[...], low_ref[...], order, keep_ref)


def eliminate(work_ref, k):
    n = work_ref.shape[0]
    size = PANEL
    lane = iota((size, n), 1)
    row_wide = iota((size, n), 0)
    row = iota((size, 128), 0)
    first = pl.multiple_of(k * size, size)
    rows = work_ref[pl.ds(first, size), :]
    slab = rows[:, 0:128]
    for g in range(1, n // 128):
        slab = jnp.where(first >= g * 128, rows[:, g * 128 : (g + 1) * 128], slab)
    slab = pltpu.roll(slab, (128 - first % 128) % 128, 1)
    columns = [jnp.broadcast_to(slab[:, j : j + 1], (size, 128)) for j in range(size)]
    scale = jnp.zeros((size, 128), f32)
    for j in range(size):
        pivot = columns[j][j : j + 1, :]
        scale = jnp.where(row == j, lax.rsqrt(pivot), scale)
        factor = jnp.where(row > j, columns[j] * (1.0 / pivot), 0.0)
        for l in range(j + 1, size):
            columns[l] = columns[l] - factor * columns[l][j : j + 1, :]
        rows = jnp.where(lane == first + j, jnp.where(row_wide == j, 1.0, 0.0), rows)
        rows = rows - jnp.concatenate([factor] * (n // 128), axis=1) * rows[j : j + 1, :]
    rows = rows * jnp.concatenate([scale] * (n // 128), axis=1)
    upper = jnp.where(lane >= first + size, rows, 0.0)
    update = tn(upper, rows, HIGHEST)
    full_lane, full_row = iota((n, n), 1), iota((n, n), 0)
    stale = (full_row >= first + size) & (full_lane >= first) & (full_lane < first + size)
    work_ref[...] = jnp.where(stale, 0.0, work_ref[...]) - update
    work_ref[pl.ds(first, size), :] = rows


def inverse_kernel(start, stop):
    def kernel(*refs):
        work_ref = refs[-1]
        n = work_ref.shape[0]
        if start == 0:
            pivot_x, pivot_hi, pivot_lo = [ref[...] for ref in refs[:3]]
            width = pivot_x.shape[1]
            wide = pivot_x.astype(f32)
            square = wide * wide
            left = jnp.sum(square, axis=1, keepdims=True)
            right = nt(jnp.ones((8, width), f32), square, HIGHEST)[0:1, :]
            product = nt(pivot_hi, pivot_hi) + (nt(pivot_lo, pivot_hi) + nt(pivot_hi, pivot_lo))
            work_ref[...] = mixed(nt(pivot_x, pivot_x), left, right, width) - product
        else:
            work_ref[...] = refs[0][...]

        def panel(k, carry):
            eliminate(work_ref, k)
            return carry

        lax.fori_loop(start, stop, panel, 0)
        if stop == n // PANEL:
            work_ref[...] = jnp.where(iota((n, n), 1) <= iota((n, n), 0), work_ref[...], 0.0)

    return kernel


def columns_kernel(residual_ref, inverse_ref, out_ref):
    out_ref[...] = dot(residual_ref[...], inverse_ref[...], 0, 1, HIGHEST)


def rows_kernel(masks, rank_ref, *refs):
    inverse_ref, out_ref, work_ref, done_ref, sems = refs[-5:]
    parts = refs[:-5]
    count = len(parts) // 2
    piece = parts[0].shape[1]
    n = inverse_ref.shape[0]
    total = done_ref.shape[1]
    depth = total - n
    middle = n // 2
    core, near_order, far_order = spots(rank_ref[0], *masks)
    for k, part in enumerate(parts):
        mine = k < count
        half = core if mine else 1 - core
        at = half * count + ((near_order if mine else far_order) ^ (k % count))
        upper = pl.ds(pl.multiple_of(at * piece, piece), piece)
        lower = pl.ds(pl.multiple_of(middle + at * piece, piece), piece)
        work_ref[upper, 0:depth] = part[0, :, 0:depth]
        work_ref[lower, 0:depth] = part[0, :, depth : 2 * depth]
        work_ref[upper, depth:] = part[0, :, 2 * depth : 2 * depth + n]
        work_ref[lower, depth + middle :] = part[0, :, 2 * depth + n :]
    inverse = inverse_ref[...]
    corner = work_ref[0:middle, depth + middle :]
    first = nn(inverse[:, 0:middle], work_ref[0:middle, depth : depth + middle], HIGHEST) + nt(
        inverse[:, middle:], corner, HIGHEST
    )
    second = nn(inverse, work_ref[:, depth + middle :], HIGHEST)
    done_ref[:, depth:] = nt(jnp.concatenate([first, second], axis=1), inverse, HIGHEST)
    copies = []

    def send(here):
        copy = pltpu.make_async_copy(
            done_ref.at[:, here], out_ref.at[:, here], sems.at[len(copies)]
        )
        copies.append(copy)
        copy.start()

    send(slice(depth, total))
    for at in range(0, depth, depth // 4):
        here = slice(at, at + depth // 4)
        done_ref[:, here] = nn(inverse, work_ref[:, here], HIGHEST)
        send(here)
    for copy in copies:
        copy.wait()


def body(features, factor, ip_weights, pivot_owner, pivot_position):
    axes = ("row", "col")
    n_row, n_col = lax.axis_size("row"), lax.axis_size("col")
    devices = n_row * n_col
    row_bits, col_bits = n_row.bit_length() - 1, n_col.bit_length() - 1
    assert n_row == 1 << row_bits and n_col == 1 << col_bits and row_bits >= 2 and col_bits >= 1
    col_low = 1
    core = n_col
    side = 2 * n_col
    masks = (core, side, col_low)
    others = [n_col << k for k in range(2, row_bits)] + [1 << k for k in range(1, col_bits)]
    others = others[::-1]
    rank = (lax.axis_index("row") * n_col + lax.axis_index("col")).astype(i32)[None]
    pivots = pivot_owner.shape[0]
    slots = 2 * pivots // devices + 2
    rows, width = features.shape
    depth = factor.shape[1]
    samples = rows * devices
    total = depth + pivots

    def pair(mask):
        return [(i, i ^ mask) for i in range(devices)]

    def staggered(mask_zero, mask_one):
        return [(i, i ^ (mask_one if i & core else mask_zero)) for i in range(devices)]

    first_pair = staggered(side, col_low)
    second_pair = staggered(col_low, side)
    both_pair = pair(side | col_low)
    core_pair = pair(core)

    def move(value, perm):
        return lax.ppermute(value, axes, perm)

    def tie(*values):
        return lax.optimization_barrier(values)

    owner_row = pivot_owner[None, :]
    far = lambda x: pltpu.with_memory_space_constraint(x, pltpu.HBM)
    listed = (1, pivots)
    held_x, held_h, kept, factor_near = pl.pallas_call(
        pick_kernel,
        out_shape=(
            pltpu.VMEM((slots, width), bf16),
            pltpu.VMEM((slots, depth), jnp.int16),
            pltpu.VMEM((rows, width), bf16),
            pltpu.VMEM((rows, depth), f32),
        ),
        in_specs=[pl.BlockSpec(memory_space=pltpu.SMEM)] + [pl.BlockSpec(memory_space=pltpu.HBM)] * 4,
        out_specs=tuple(pl.BlockSpec(memory_space=pltpu.VMEM) for _ in range(4)),
        scratch_shapes=[
            pltpu.VMEM(listed, i32),
            pltpu.VMEM(listed, i32),
            pltpu.SMEM(listed, i32),
            pltpu.SMEM(listed, i32),
            pltpu.SMEM((slots + 1,), i32),
            pltpu.VMEM((slots, depth), f32),
            pltpu.SemaphoreType.DMA((7,)),
        ],
        compiler_params=pltpu.CompilerParams(vmem_limit_bytes=24 << 20),
    )(rank, far(owner_row), far(pivot_position[None, :]), far(features), far(factor))

    def joined(one, two):
        shape = (2 * one.shape[0], one.shape[1])
        return call(join_kernel, pltpu.VMEM(shape, one.dtype), one, two)

    prepared = False
    perms = [pair(mask) for mask in others] + [first_pair]
    for perm in perms:
        got_h = near(move(held_h, perm))
        got_x = near(move(held_x, perm))
        if not prepared:
            source, norm, high, low = call(
                prepare_kernel(core, side, col_low, others, slots, devices),
                (
                    pltpu.VMEM((1, pivots), i32),
                    pltpu.VMEM((1, rows), f32),
                    pltpu.VMEM((rows, depth), bf16),
                    pltpu.VMEM((rows, depth), bf16),
                ),
                rank, owner_row, kept, factor_near, smem=1,
            )
            got_h, got_x, source, norm, high, low = tie(got_h, got_x, source, norm, high, low)
            prepared = True
        held_h = joined(held_h, got_h)
        held_x = joined(held_x, got_x)
    across_h = near(move(held_h, second_pair))
    across_x = near(move(held_x, second_pair))
    far_h, far_x = near(move(held_h, core_pair)), near(move(held_x, core_pair))
    plane = pltpu.VMEM((pivots, depth), bf16)
    pivot_x, coarse, fine = call(
        order_kernel,
        (pltpu.VMEM((pivots, width), bf16), plane, plane),
        source, held_x, held_h, far_x, far_h,
    )
    across_h, coarse, fine = tie(across_h, coarse, fine)
    beyond_h = near(move(across_h, core_pair))
    coarse, fine = call(partial(across_kernel, 1), (plane, plane), source, across_h, coarse, fine)
    coarse, fine = call(partial(across_kernel, 3), (plane, plane), source, beyond_h, coarse, fine)
    across_x, coarse, fine = tie(across_x, coarse, fine)
    beyond_x = near(move(across_x, core_pair))
    product = call(product_kernel, pltpu.VMEM((pivots, rows), f32), coarse, fine, high, low)
    beyond_x, product = tie(beyond_x, product)

    weights = ip_weights[None, :]
    half = pltpu.VMEM((4, pivots // 16, 2 * depth + pivots + pivots // 2), f32)
    pivot_x, residual, send = call(
        partial(residual_kernel, masks, samples),
        (pltpu.VMEM((pivots, width), bf16), pltpu.VMEM((pivots, rows), f32), half),
        rank, source, pivot_x, across_x, beyond_x, product, kept, high, low, norm, weights,
        smem=1,
    )
    received = move(send, core_pair)
    keep = call(partial(keep_kernel, masks, samples), half, rank, residual, high, low, weights, smem=1)
    keep = keep + received

    panels = pivots // PANEL
    cuts = [0, panels // 4, panels * 5 // 8, panels]

    def eliminate_step(step, *given):
        return call(
            inverse_kernel(cuts[step], cuts[step + 1]), pltpu.VMEM((pivots, pivots), f32), *given
        )

    keep, pivot_x, coarse, fine = tie(keep, pivot_x, coarse, fine)
    from_both = move(keep[3:4], both_pair)
    from_second = move(keep[1:2], second_pair)
    from_first = move(keep[2:3], first_pair)
    work = eliminate_step(0, pivot_x, coarse, fine)
    from_both, from_second, from_first, work = tie(from_both, from_second, from_first, work)
    keep = (keep[0:1] + from_both) + (from_second + from_first)
    step = 1
    for mask in others:
        got = move(keep, pair(mask))
        if step < len(cuts) - 1:
            work = eliminate_step(step, work)
            got, work = tie(got, work)
            step += 1
        keep = keep + got
    inverse = work
    keep, inverse = tie(keep, inverse)
    pieces = [near(keep)] + [near(move(keep, perm)) for perm in (second_pair, first_pair, both_pair)]
    new_columns = call(columns_kernel, jax.ShapeDtypeStruct((rows, pivots), f32), residual, inverse)
    pieces[3], new_columns = tie(pieces[3], new_columns)
    pieces += [near(move(piece, core_pair)) for piece in pieces]
    gram_rows = pl.pallas_call(
        partial(rows_kernel, masks),
        out_shape=jax.ShapeDtypeStruct((pivots, total), f32),
        in_specs=[pl.BlockSpec(memory_space=pltpu.SMEM)] + [pl.BlockSpec(memory_space=pltpu.VMEM)] * 9,
        out_specs=pl.BlockSpec(memory_space=pltpu.HBM),
        scratch_shapes=[
            pltpu.VMEM((pivots, total), f32),
            pltpu.VMEM((pivots, total), f32),
            pltpu.SemaphoreType.DMA((5,)),
        ],
        compiler_params=pltpu.CompilerParams(vmem_limit_bytes=24 << 20),
    )(rank, *pieces, inverse)
    return (new_columns, gram_rows)


def solution(mesh):
    placed = (P(("row", "col"), None), P(("row", "col"), None), P(("row", "col")), P(), P())

    return jax.shard_map(
        body, mesh=mesh, in_specs=placed, out_specs=(P(("row", "col"), None), P()), check_vma=False
    )
```

```python
from functools import partial

import jax
import jax.numpy as jnp
from jax import lax
from jax.experimental import pallas as pl
from jax.experimental.pallas import tpu as pltpu
from jax.sharding import PartitionSpec as P


HIGHEST = lax.Precision.HIGHEST
f32 = jnp.float32
bf16 = jnp.bfloat16
i32 = jnp.int32
PANEL = 32
STEPS = 2.0**20


def dot(a, b, left, right, precision=None):
    return lax.dot_general(
        a, b, (((left,), (right,)), ((), ())), precision=precision, preferred_element_type=f32
    )


def nn(a, b, precision=None):
    return dot(a, b, 1, 0, precision)


def nt(a, b, precision=None):
    return dot(a, b, 1, 1, precision)


def tn(a, b, precision=None):
    return dot(a, b, 0, 0, precision)


def split(a):
    high = a.astype(bf16)
    low = (a - high.astype(f32)).astype(bf16)
    return high, low


def near(x):
    return pltpu.with_memory_space_constraint(x, pltpu.VMEM)


def call(kernel, outs, *args, smem=0, scratch=(), flops=10**9):
    specs = [pl.BlockSpec(memory_space=pltpu.SMEM)] * smem + [
        pl.BlockSpec(memory_space=pltpu.VMEM)
    ] * (len(args) - smem)
    return pl.pallas_call(
        kernel,
        out_shape=outs,
        in_specs=specs,
        out_specs=jax.tree.map(lambda _: pl.BlockSpec(memory_space=pltpu.VMEM), outs),
        scratch_shapes=scratch,
        compiler_params=pltpu.CompilerParams(vmem_limit_bytes=24 << 20),
        cost_estimate=pl.CostEstimate(flops=flops, transcendentals=0, bytes_accessed=10**6),
    )(*args)


def onehot(mask):
    return jnp.where(mask, 1.0, 0.0).astype(bf16)


def iota(shape, axis):
    return lax.broadcasted_iota(i32, shape, axis)


def pick_kernel(
    rank_ref, owner_ref, position_ref, features_ref, factor_ref,
    slots_x_ref, slots_h_ref, kept_ref, factor_in,
    owner_in, position_in, owner_list, position_list, found, rows_in, sems,
):
    slots = slots_x_ref.shape[0]
    pivots = owner_ref.shape[1]
    rows = features_ref.shape[0]
    half = rows // 2
    pairs = [
        (owner_ref, owner_list),
        (position_ref, position_list),
        (owner_ref, owner_in),
        (position_ref, position_in),
        (features_ref, kept_ref),
        (factor_ref.at[pl.ds(0, half), :], factor_in.at[pl.ds(0, half), :]),
        (factor_ref.at[pl.ds(half, half), :], factor_in.at[pl.ds(half, half), :]),
    ]
    copies = [
        pltpu.make_async_copy(source, target, sems.at[k]) for k, (source, target) in enumerate(pairs)
    ]
    for copy in copies:
        copy.start()
    rank = rank_ref[0]
    for k in range(slots + 1):
        found[k] = 0
    copies[0].wait()
    copies[1].wait()

    def collect(k, count):
        for p in range(8):
            at = k * 8 + p
            found[count] = position_list[0, at]
            count = jnp.minimum(count + (owner_list[0, at] == rank).astype(i32), slots)
        return count

    lax.fori_loop(0, pivots // 8, collect, jnp.int32(0))
    ahead = onehot(iota((pivots, pivots), 0) < iota((pivots, pivots), 1))
    copies[2].wait()
    mine = owner_in[...] == rank
    mine_rows = jnp.broadcast_to(jnp.where(mine, 1.0, 0.0), (8, pivots)).astype(bf16)
    order = nn(mine_rows, ahead)[0:1, :].astype(i32)
    chosen = onehot((iota((slots, pivots), 0) == order) & mine)
    copies[3].wait()
    located = onehot(iota((rows, pivots), 0) == position_in[...])
    take = nt(chosen, located).astype(bf16)
    copies[4].wait()
    slots_x_ref[...] = nn(take, kept_ref[...]).astype(bf16)
    copies[5].wait()
    copies[6].wait()
    for k in range(slots):
        rows_in[k : k + 1, :] = factor_in[pl.ds(found[k], 1), :]
    slots_h_ref[...] = jnp.round(rows_in[...] * STEPS).astype(i32).astype(jnp.int16)


def prepare_kernel(core, side, col_low, others, slots, devices):
    def kernel(
        rank_ref, owner_ref, features_ref, factor_ref, source_ref, norm_ref, high_ref, low_ref
    ):
        pivots = owner_ref.shape[1]
        owner = owner_ref[...]
        ahead = onehot(iota((pivots, pivots), 0) < iota((pivots, pivots), 1))
        owned = iota((devices, pivots), 0) == owner
        counts = nn(onehot(owned), ahead)
        slot_rank = jnp.sum(jnp.where(owned, counts, 0.0), axis=0, keepdims=True).astype(i32)
        apart = owner ^ rank_ref[0]
        bit = lambda mask: (apart >> (mask.bit_length() - 1)) & 1
        place = jnp.zeros_like(apart)
        for k, mask in enumerate(others):
            place = place + (bit(mask) << k)
        at = len(others)
        low_core = (owner & core) == 0
        lead = jnp.where(low_core, bit(side), bit(col_low))
        trail = jnp.where(low_core, bit(col_low), bit(side))
        place = place + (lead << at) + (trail << (at + 1)) + (bit(core) << (at + 2))
        source_ref[...] = place * slots + slot_rank
        high, low = split(factor_ref[...])
        high_ref[...] = high
        low_ref[...] = low
        wide = features_ref[...].astype(f32)
        norm_ref[...] = nt(jnp.ones((8, wide.shape[1]), f32), wide * wide, HIGHEST)[0:1, :]

    return kernel


def mixed(cross, left, right, width):
    base = jnp.exp((left + right - 2.0 * cross) * (-0.25 / width))
    square = base * base
    return 0.5 * base + 0.3 * square + 0.2 * (square * square)


def join_kernel(*refs):
    out_ref = refs[-1]
    at = 0
    for ref in refs[:-1]:
        out_ref[at : at + ref.shape[0]] = ref[...]
        at += ref.shape[0]


def spots(rank, core, side, col_low):
    bit = lambda mask: (rank >> (mask.bit_length() - 1)) & 1
    lead = jnp.where(bit(core) == 0, bit(side), bit(col_low))
    trail = jnp.where(bit(core) == 0, bit(col_low), bit(side))
    return bit(core), lead * 2 + trail, trail * 2 + lead


def gram_half(residual_ref, half, weights, high, low, order, out_ref):
    count, piece, _ = out_ref.shape
    size = count * piece
    depth = high.shape[1]
    n = residual_ref.shape[0]
    upper = residual_ref[pl.ds(pl.multiple_of(half * size, size), size), :]
    lower = residual_ref[pl.ds(pl.multiple_of(n // 2 + half * size, size), size), :]
    weighted = jnp.concatenate([upper, lower], axis=0) * weights
    weighted_hi, weighted_lo = split(weighted)
    left = nn(weighted_hi, high) + (nn(weighted_lo, high) + nn(weighted_hi, low))
    residual = residual_ref[...]
    top = nt(weighted[0:size], residual, HIGHEST)
    bottom = nt(weighted[size:], residual[n // 2 :], HIGHEST)
    for p in range(count):
        spot = (order & (count - 1)) ^ p
        rows = slice(p * piece, (p + 1) * piece)
        out_ref[spot, :, 0:depth] = left[rows]
        out_ref[spot, :, depth : 2 * depth] = left[size + p * piece : size + (p + 1) * piece]
        out_ref[spot, :, 2 * depth : 2 * depth + n] = top[rows]
        out_ref[spot, :, 2 * depth + n :] = bottom[rows]


def chosen_rows(source, start, held):
    return onehot(iota((held, source.shape[1]), 0) == source - start)


def ordered_h(source, start, h_ref):
    chosen = chosen_rows(source, start, h_ref.shape[0])
    q = h_ref[...].astype(i32)
    coarse = (q + 128) >> 8
    fine = q - (coarse << 8)
    coarse = (coarse.astype(f32) * (256 / STEPS)).astype(bf16)
    fine = (fine.astype(f32) * (1 / STEPS)).astype(bf16)
    return tn(chosen, coarse), tn(chosen, fine)


def ordered_x(source, start, x_ref):
    return tn(chosen_rows(source, start, x_ref.shape[0]), x_ref[...])


def order_kernel(source_ref, a_x_ref, a_h_ref, c_x_ref, c_h_ref, x_ref, coarse_ref, fine_ref):
    held = a_x_ref.shape[0]
    source = source_ref[...]
    x_ref[...] = (
        ordered_x(source, 0, a_x_ref) + ordered_x(source, 2 * held, c_x_ref)
    ).astype(bf16)
    one, two = ordered_h(source, 0, a_h_ref), ordered_h(source, 2 * held, c_h_ref)
    coarse_ref[...] = (one[0] + two[0]).astype(bf16)
    fine_ref[...] = (one[1] + two[1]).astype(bf16)


def across_kernel(place, source_ref, h_ref, coarse_in, fine_in, coarse_ref, fine_ref):
    coarse, fine = ordered_h(source_ref[...], place * h_ref.shape[0], h_ref)
    coarse_ref[...] = (coarse_in[...].astype(f32) + coarse).astype(bf16)
    fine_ref[...] = (fine_in[...].astype(f32) + fine).astype(bf16)


def product_kernel(coarse_ref, fine_ref, high_ref, low_ref, product_ref):
    coarse, high = coarse_ref[...], high_ref[...]
    product_ref[...] = nt(coarse, high) + (nt(fine_ref[...], high) + nt(coarse, low_ref[...]))


def residual_kernel(
    masks, samples, rank_ref, source_ref, x_ref, b_x_ref, d_x_ref, product_ref,
    features_ref, high_ref, low_ref, norm_ref, weights_ref, pivot_ref, residual_ref, send_ref,
):
    held, width = b_x_ref.shape
    source = source_ref[...]
    new = ordered_x(source, held, b_x_ref) + ordered_x(source, 3 * held, d_x_ref)
    pivot_x = (new + x_ref[...].astype(f32)).astype(bf16)
    pivot_ref[...] = pivot_x
    high, low = high_ref[...], low_ref[...]
    pivot_wide = pivot_x.astype(f32)
    pivot_norm = jnp.sum(pivot_wide * pivot_wide, axis=1, keepdims=True)
    residual_ref[...] = (
        mixed(nt(pivot_x, features_ref[...]), pivot_norm, norm_ref[...], width) - product_ref[...]
    )
    core, _, order = spots(rank_ref[0], *masks)
    weights = weights_ref[...] / samples
    gram_half(residual_ref, 1 - core, weights, high, low, order, send_ref)


def keep_kernel(masks, samples, rank_ref, residual_ref, high_ref, low_ref, weights_ref, keep_ref):
    core, order, _ = spots(rank_ref[0], *masks)
    weights = weights_ref[...] / samples
    gram_half(residual_ref, core, weights, high_ref[...], low_ref[...], order, keep_ref)


def eliminate(work_ref, k):
    n = work_ref.shape[0]
    size = PANEL
    lane = iota((size, n), 1)
    row_wide = iota((size, n), 0)
    row = iota((size, 128), 0)
    first = pl.multiple_of(k * size, size)
    rows = work_ref[pl.ds(first, size), :]
    slab = rows[:, 0:128]
    for g in range(1, n // 128):
        slab = jnp.where(first >= g * 128, rows[:, g * 128 : (g + 1) * 128], slab)
    slab = pltpu.roll(slab, (128 - first % 128) % 128, 1)
    columns = [jnp.broadcast_to(slab[:, j : j + 1], (size, 128)) for j in range(size)]
    scale = jnp.zeros((size, 128), f32)
    for j in range(size):
        pivot = columns[j][j : j + 1, :]
        scale = jnp.where(row == j, lax.rsqrt(pivot), scale)
        factor = jnp.where(row > j, columns[j] * (1.0 / pivot), 0.0)
        for l in range(j + 1, size):
            columns[l] = columns[l] - factor * columns[l][j : j + 1, :]
        rows = jnp.where(lane == first + j, jnp.where(row_wide == j, 1.0, 0.0), rows)
        rows = rows - jnp.concatenate([factor] * (n // 128), axis=1) * rows[j : j + 1, :]
    rows = rows * jnp.concatenate([scale] * (n // 128), axis=1)
    upper = jnp.where(lane >= first + size, rows, 0.0)
    update = tn(upper, rows, HIGHEST)
    full_lane, full_row = iota((n, n), 1), iota((n, n), 0)
    stale = (full_row >= first + size) & (full_lane >= first) & (full_lane < first + size)
    work_ref[...] = jnp.where(stale, 0.0, work_ref[...]) - update
    work_ref[pl.ds(first, size), :] = rows


def inverse_kernel(start, stop):
    def kernel(*refs):
        work_ref = refs[-1]
        n = work_ref.shape[0]
        if start == 0:
            pivot_x, pivot_hi, pivot_lo = [ref[...] for ref in refs[:3]]
            width = pivot_x.shape[1]
            wide = pivot_x.astype(f32)
            square = wide * wide
            left = jnp.sum(square, axis=1, keepdims=True)
            right = nt(jnp.ones((8, width), f32), square, HIGHEST)[0:1, :]
            product = nt(pivot_hi, pivot_hi) + (nt(pivot_lo, pivot_hi) + nt(pivot_hi, pivot_lo))
            work_ref[...] = mixed(nt(pivot_x, pivot_x), left, right, width) - product
        else:
            work_ref[...] = refs[0][...]

        def panel(k, carry):
            eliminate(work_ref, k)
            return carry

        lax.fori_loop(start, stop, panel, 0)
        if stop == n // PANEL:
            work_ref[...] = jnp.where(iota((n, n), 1) <= iota((n, n), 0), work_ref[...], 0.0)

    return kernel


def columns_kernel(residual_ref, inverse_ref, out_ref):
    out_ref[...] = dot(residual_ref[...], inverse_ref[...], 0, 1, HIGHEST)


def rows_kernel(masks, rank_ref, *refs):
    inverse_ref, out_ref, work_ref, done_ref, sems = refs[-5:]
    parts = refs[:-5]
    count = len(parts) // 2
    piece = parts[0].shape[1]
    n = inverse_ref.shape[0]
    total = done_ref.shape[1]
    depth = total - n
    middle = n // 2
    core, near_order, far_order = spots(rank_ref[0], *masks)
    for k, part in enumerate(parts):
        mine = k < count
        half = core if mine else 1 - core
        at = half * count + ((near_order if mine else far_order) ^ (k % count))
        upper = pl.ds(pl.multiple_of(at * piece, piece), piece)
        lower = pl.ds(pl.multiple_of(middle + at * piece, piece), piece)
        work_ref[upper, 0:depth] = part[0, :, 0:depth]
        work_ref[lower, 0:depth] = part[0, :, depth : 2 * depth]
        work_ref[upper, depth:] = part[0, :, 2 * depth : 2 * depth + n]
        work_ref[lower, depth + middle :] = part[0, :, 2 * depth + n :]
    inverse = inverse_ref[...]
    corner = work_ref[0:middle, depth + middle :]
    first = nn(inverse[:, 0:middle], work_ref[0:middle, depth : depth + middle], HIGHEST) + nt(
        inverse[:, middle:], corner, HIGHEST
    )
    second = nn(inverse, work_ref[:, depth + middle :], HIGHEST)
    done_ref[:, depth:] = nt(jnp.concatenate([first, second], axis=1), inverse, HIGHEST)
    copies = []

    def send(here):
        copy = pltpu.make_async_copy(
            done_ref.at[:, here], out_ref.at[:, here], sems.at[len(copies)]
        )
        copies.append(copy)
        copy.start()

    send(slice(depth, total))
    for at in range(0, depth, depth // 4):
        here = slice(at, at + depth // 4)
        done_ref[:, here] = nn(inverse, work_ref[:, here], HIGHEST)
        send(here)
    for copy in copies:
        copy.wait()


def body(features, factor, ip_weights, pivot_owner, pivot_position):
    axes = ("row", "col")
    n_row, n_col = lax.axis_size("row"), lax.axis_size("col")
    devices = n_row * n_col
    row_bits, col_bits = n_row.bit_length() - 1, n_col.bit_length() - 1
    assert n_row == 1 << row_bits and n_col == 1 << col_bits and row_bits >= 2 and col_bits >= 1
    col_low = 1
    core = n_col
    side = 2 * n_col
    masks = (core, side, col_low)
    others = [n_col << k for k in range(2, row_bits)] + [1 << k for k in range(1, col_bits)]
    others = others[::-1]
    rank = (lax.axis_index("row") * n_col + lax.axis_index("col")).astype(i32)[None]
    pivots = pivot_owner.shape[0]
    slots = 2 * pivots // devices + 2
    rows, width = features.shape
    depth = factor.shape[1]
    samples = rows * devices
    total = depth + pivots

    def pair(mask):
        return [(i, i ^ mask) for i in range(devices)]

    def staggered(mask_zero, mask_one):
        return [(i, i ^ (mask_one if i & core else mask_zero)) for i in range(devices)]

    first_pair = staggered(side, col_low)
    second_pair = staggered(col_low, side)
    both_pair = pair(side | col_low)
    core_pair = pair(core)

    def move(value, perm):
        return lax.ppermute(value, axes, perm)

    def tie(*values):
        return lax.optimization_barrier(values)

    owner_row = pivot_owner[None, :]
    far = lambda x: pltpu.with_memory_space_constraint(x, pltpu.HBM)
    listed = (1, pivots)
    held_x, held_h, kept, factor_near = pl.pallas_call(
        pick_kernel,
        out_shape=(
            pltpu.VMEM((slots, width), bf16),
            pltpu.VMEM((slots, depth), jnp.int16),
            pltpu.VMEM((rows, width), bf16),
            pltpu.VMEM((rows, depth), f32),
        ),
        in_specs=[pl.BlockSpec(memory_space=pltpu.SMEM)] + [pl.BlockSpec(memory_space=pltpu.HBM)] * 4,
        out_specs=tuple(pl.BlockSpec(memory_space=pltpu.VMEM) for _ in range(4)),
        scratch_shapes=[
            pltpu.VMEM(listed, i32),
            pltpu.VMEM(listed, i32),
            pltpu.SMEM(listed, i32),
            pltpu.SMEM(listed, i32),
            pltpu.SMEM((slots + 1,), i32),
            pltpu.VMEM((slots, depth), f32),
            pltpu.SemaphoreType.DMA((7,)),
        ],
        compiler_params=pltpu.CompilerParams(vmem_limit_bytes=24 << 20),
    )(rank, far(owner_row), far(pivot_position[None, :]), far(features), far(factor))

    def joined(one, two):
        shape = (2 * one.shape[0], one.shape[1])
        return call(join_kernel, pltpu.VMEM(shape, one.dtype), one, two)

    prepared = False
    perms = [pair(mask) for mask in others] + [first_pair]
    for perm in perms:
        got_h = near(move(held_h, perm))
        got_x = near(move(held_x, perm))
        if not prepared:
            source, norm, high, low = call(
                prepare_kernel(core, side, col_low, others, slots, devices),
                (
                    pltpu.VMEM((1, pivots), i32),
                    pltpu.VMEM((1, rows), f32),
                    pltpu.VMEM((rows, depth), bf16),
                    pltpu.VMEM((rows, depth), bf16),
                ),
                rank, owner_row, kept, factor_near, smem=1,
            )
            got_h, got_x, source, norm, high, low = tie(got_h, got_x, source, norm, high, low)
            prepared = True
        held_h = joined(held_h, got_h)
        held_x = joined(held_x, got_x)
    across_h = near(move(held_h, second_pair))
    across_x = near(move(held_x, second_pair))
    far_h, far_x = near(move(held_h, core_pair)), near(move(held_x, core_pair))
    plane = pltpu.VMEM((pivots, depth), bf16)
    pivot_x, coarse, fine = call(
        order_kernel,
        (pltpu.VMEM((pivots, width), bf16), plane, plane),
        source, held_x, held_h, far_x, far_h,
    )
    across_h, coarse, fine = tie(across_h, coarse, fine)
    beyond_h = near(move(across_h, core_pair))
    coarse, fine = call(partial(across_kernel, 1), (plane, plane), source, across_h, coarse, fine)
    coarse, fine = call(partial(across_kernel, 3), (plane, plane), source, beyond_h, coarse, fine)
    across_x, coarse, fine = tie(across_x, coarse, fine)
    beyond_x = near(move(across_x, core_pair))
    product = call(product_kernel, pltpu.VMEM((pivots, rows), f32), coarse, fine, high, low)
    beyond_x, product = tie(beyond_x, product)

    weights = ip_weights[None, :]
    half = pltpu.VMEM((4, pivots // 16, 2 * depth + pivots + pivots // 2), f32)
    pivot_x, residual, send = call(
        partial(residual_kernel, masks, samples),
        (pltpu.VMEM((pivots, width), bf16), pltpu.VMEM((pivots, rows), f32), half),
        rank, source, pivot_x, across_x, beyond_x, product, kept, high, low, norm, weights,
        smem=1,
    )
    received = move(send, core_pair)
    keep = call(partial(keep_kernel, masks, samples), half, rank, residual, high, low, weights, smem=1)
    keep = keep + received

    panels = pivots // PANEL
    cuts = [0, panels * 3 // 8, panels * 3 // 4, panels]

    def eliminate_step(step, *given):
        return call(
            inverse_kernel(cuts[step], cuts[step + 1]), pltpu.VMEM((pivots, pivots), f32), *given
        )

    keep, pivot_x, coarse, fine = tie(keep, pivot_x, coarse, fine)
    from_both = move(keep[3:4], both_pair)
    from_second = move(keep[1:2], second_pair)
    from_first = move(keep[2:3], first_pair)
    work = eliminate_step(0, pivot_x, coarse, fine)
    from_both, from_second, from_first, work = tie(from_both, from_second, from_first, work)
    keep = (keep[0:1] + from_both) + (from_second + from_first)
    step = 1
    split_at = keep.shape[1] // 2
    one, two = keep[:, :split_at], keep[:, split_at:]
    for mask, other_mask in zip(others, others[::-1]):
        got_one, got_two = move(one, pair(mask)), move(two, pair(other_mask))
        if step < len(cuts) - 1:
            work = eliminate_step(step, work)
            got_one, got_two, work = tie(got_one, got_two, work)
            step += 1
        one, two = one + got_one, two + got_two
    keep = jnp.concatenate([one, two], axis=1)
    inverse = work
    keep, inverse = tie(keep, inverse)
    pieces = [near(keep)] + [near(move(keep, perm)) for perm in (second_pair, first_pair, both_pair)]
    new_columns = call(columns_kernel, jax.ShapeDtypeStruct((rows, pivots), f32), residual, inverse)
    pieces[3], new_columns = tie(pieces[3], new_columns)
    pieces += [near(move(piece, core_pair)) for piece in pieces]
    gram_rows = pl.pallas_call(
        partial(rows_kernel, masks),
        out_shape=jax.ShapeDtypeStruct((pivots, total), f32),
        in_specs=[pl.BlockSpec(memory_space=pltpu.SMEM)] + [pl.BlockSpec(memory_space=pltpu.VMEM)] * 9,
        out_specs=pl.BlockSpec(memory_space=pltpu.HBM),
        scratch_shapes=[
            pltpu.VMEM((pivots, total), f32),
            pltpu.VMEM((pivots, total), f32),
            pltpu.SemaphoreType.DMA((5,)),
        ],
        compiler_params=pltpu.CompilerParams(vmem_limit_bytes=24 << 20),
    )(rank, *pieces, inverse)
    return (new_columns, gram_rows)


def solution(mesh):
    placed = (P(("row", "col"), None), P(("row", "col"), None), P(("row", "col")), P(), P())

    return jax.shard_map(
        body, mesh=mesh, in_specs=placed, out_specs=(P(("row", "col"), None), P()), check_vma=False
    )
```

```python
from functools import partial

import jax
import jax.numpy as jnp
from jax import lax
from jax.experimental import pallas as pl
from jax.experimental.pallas import tpu as pltpu
from jax.sharding import PartitionSpec as P


HIGHEST = lax.Precision.HIGHEST
f32 = jnp.float32
bf16 = jnp.bfloat16
i32 = jnp.int32
PANEL = 32
STEPS = 2.0**20


def dot(a, b, left, right, precision=None):
    return lax.dot_general(
        a, b, (((left,), (right,)), ((), ())), precision=precision, preferred_element_type=f32
    )


def nn(a, b, precision=None):
    return dot(a, b, 1, 0, precision)


def nt(a, b, precision=None):
    return dot(a, b, 1, 1, precision)


def tn(a, b, precision=None):
    return dot(a, b, 0, 0, precision)


def split(a):
    high = a.astype(bf16)
    low = (a - high.astype(f32)).astype(bf16)
    return high, low


def near(x):
    return pltpu.with_memory_space_constraint(x, pltpu.VMEM)


def call(kernel, outs, *args, smem=0, scratch=(), flops=10**9):
    specs = [pl.BlockSpec(memory_space=pltpu.SMEM)] * smem + [
        pl.BlockSpec(memory_space=pltpu.VMEM)
    ] * (len(args) - smem)
    return pl.pallas_call(
        kernel,
        out_shape=outs,
        in_specs=specs,
        out_specs=jax.tree.map(lambda _: pl.BlockSpec(memory_space=pltpu.VMEM), outs),
        scratch_shapes=scratch,
        compiler_params=pltpu.CompilerParams(vmem_limit_bytes=24 << 20),
        cost_estimate=pl.CostEstimate(flops=flops, transcendentals=0, bytes_accessed=10**6),
    )(*args)


def onehot(mask):
    return jnp.where(mask, 1.0, 0.0).astype(bf16)


def iota(shape, axis):
    return lax.broadcasted_iota(i32, shape, axis)


def pick_kernel(
    rank_ref, owner_ref, position_ref, features_ref, factor_ref,
    slots_x_ref, slots_h_ref, kept_ref, factor_in,
    owner_in, position_in, owner_list, position_list, found, rows_in, sems,
):
    slots = slots_x_ref.shape[0]
    pivots = owner_ref.shape[1]
    rows = features_ref.shape[0]
    half = rows // 2
    pairs = [
        (owner_ref, owner_list),
        (position_ref, position_list),
        (owner_ref, owner_in),
        (position_ref, position_in),
        (features_ref, kept_ref),
        (factor_ref.at[pl.ds(0, half), :], factor_in.at[pl.ds(0, half), :]),
        (factor_ref.at[pl.ds(half, half), :], factor_in.at[pl.ds(half, half), :]),
    ]
    copies = [
        pltpu.make_async_copy(source, target, sems.at[k]) for k, (source, target) in enumerate(pairs)
    ]
    for copy in copies:
        copy.start()
    rank = rank_ref[0]
    for k in range(slots + 1):
        found[k] = 0
    copies[0].wait()
    copies[1].wait()

    def collect(k, count):
        for p in range(8):
            at = k * 8 + p
            found[count] = position_list[0, at]
            count = jnp.minimum(count + (owner_list[0, at] == rank).astype(i32), slots)
        return count

    lax.fori_loop(0, pivots // 8, collect, jnp.int32(0))
    ahead = onehot(iota((pivots, pivots), 0) < iota((pivots, pivots), 1))
    copies[2].wait()
    mine = owner_in[...] == rank
    mine_rows = jnp.broadcast_to(jnp.where(mine, 1.0, 0.0), (8, pivots)).astype(bf16)
    order = nn(mine_rows, ahead)[0:1, :].astype(i32)
    chosen = onehot((iota((slots, pivots), 0) == order) & mine)
    copies[3].wait()
    located = onehot(iota((rows, pivots), 0) == position_in[...])
    take = nt(chosen, located).astype(bf16)
    copies[4].wait()
    slots_x_ref[...] = nn(take, kept_ref[...]).astype(bf16)
    copies[5].wait()
    copies[6].wait()
    for k in range(slots):
        rows_in[k : k + 1, :] = factor_in[pl.ds(found[k], 1), :]
    slots_h_ref[...] = jnp.round(rows_in[...] * STEPS).astype(i32).astype(jnp.int16)


def prepare_kernel(core, side, col_low, others, slots, devices):
    def kernel(
        rank_ref, owner_ref, features_ref, factor_ref, source_ref, norm_ref, high_ref, low_ref
    ):
        pivots = owner_ref.shape[1]
        owner = owner_ref[...]
        ahead = onehot(iota((pivots, pivots), 0) < iota((pivots, pivots), 1))
        owned = iota((devices, pivots), 0) == owner
        counts = nn(onehot(owned), ahead)
        slot_rank = jnp.sum(jnp.where(owned, counts, 0.0), axis=0, keepdims=True).astype(i32)
        apart = owner ^ rank_ref[0]
        bit = lambda mask: (apart >> (mask.bit_length() - 1)) & 1
        at = len(others)
        low_core = (owner & core) == 0
        lead = jnp.where(low_core, bit(side), bit(col_low))
        trail = jnp.where(low_core, bit(col_low), bit(side))
        outer = (lead << at) + (trail << (at + 1)) + (bit(core) << (at + 2))
        for row, chain in enumerate((others, others[::-1])):
            place = outer
            for k, mask in enumerate(chain):
                place = place + (bit(mask) << k)
            source_ref[row : row + 1, :] = place * slots + slot_rank
        high, low = split(factor_ref[...])
        high_ref[...] = high
        low_ref[...] = low
        wide = features_ref[...].astype(f32)
        norm_ref[...] = nt(jnp.ones((8, wide.shape[1]), f32), wide * wide, HIGHEST)[0:1, :]

    return kernel


def mixed(cross, left, right, width):
    base = jnp.exp((left + right - 2.0 * cross) * (-0.25 / width))
    square = base * base
    return 0.5 * base + 0.3 * square + 0.2 * (square * square)


def join_kernel(*refs):
    out_ref = refs[-1]
    at = 0
    for ref in refs[:-1]:
        out_ref[at : at + ref.shape[0]] = ref[...]
        at += ref.shape[0]


def spots(rank, core, side, col_low):
    bit = lambda mask: (rank >> (mask.bit_length() - 1)) & 1
    lead = jnp.where(bit(core) == 0, bit(side), bit(col_low))
    trail = jnp.where(bit(core) == 0, bit(col_low), bit(side))
    return bit(core), lead * 2 + trail, trail * 2 + lead


def gram_half(residual_ref, half, weights, high, low, order, out_ref):
    count, piece, _ = out_ref.shape
    size = count * piece
    depth = high.shape[1]
    n = residual_ref.shape[0]
    upper = residual_ref[pl.ds(pl.multiple_of(half * size, size), size), :]
    lower = residual_ref[pl.ds(pl.multiple_of(n // 2 + half * size, size), size), :]
    weighted = jnp.concatenate([upper, lower], axis=0) * weights
    weighted_hi, weighted_lo = split(weighted)
    left = nn(weighted_hi, high) + (nn(weighted_lo, high) + nn(weighted_hi, low))
    residual = residual_ref[...]
    top = nt(weighted[0:size], residual, HIGHEST)
    bottom = nt(weighted[size:], residual[n // 2 :], HIGHEST)
    for p in range(count):
        spot = (order & (count - 1)) ^ p
        rows = slice(p * piece, (p + 1) * piece)
        out_ref[spot, :, 0:depth] = left[rows]
        out_ref[spot, :, depth : 2 * depth] = left[size + p * piece : size + (p + 1) * piece]
        out_ref[spot, :, 2 * depth : 2 * depth + n] = top[rows]
        out_ref[spot, :, 2 * depth + n :] = bottom[rows]


def chosen_rows(source, start, held):
    return onehot(iota((held, source.shape[1]), 0) == source - start)


def source_of(source_ref):
    return source_ref[0:1, :], source_ref[1:2, :]


def ordered_h(source, start, h_ref):
    chosen = chosen_rows(source, start, h_ref.shape[0])
    q = h_ref[...].astype(i32)
    coarse = (q + 128) >> 8
    fine = q - (coarse << 8)
    coarse = (coarse.astype(f32) * (256 / STEPS)).astype(bf16)
    fine = (fine.astype(f32) * (1 / STEPS)).astype(bf16)
    return tn(chosen, coarse), tn(chosen, fine)


def ordered_x(source, start, x_ref):
    return tn(chosen_rows(source, start, x_ref.shape[0]), x_ref[...])


def order_kernel(source_ref, a_x_ref, a_h_ref, c_x_ref, c_h_ref, x_ref, coarse_ref, fine_ref):
    held = a_x_ref.shape[0]
    source, source_x = source_of(source_ref)
    x_ref[...] = (
        ordered_x(source_x, 0, a_x_ref) + ordered_x(source_x, 2 * held, c_x_ref)
    ).astype(bf16)
    one, two = ordered_h(source, 0, a_h_ref), ordered_h(source, 2 * held, c_h_ref)
    coarse_ref[...] = (one[0] + two[0]).astype(bf16)
    fine_ref[...] = (one[1] + two[1]).astype(bf16)


def across_kernel(place, source_ref, h_ref, coarse_in, fine_in, coarse_ref, fine_ref):
    coarse, fine = ordered_h(source_of(source_ref)[0], place * h_ref.shape[0], h_ref)
    coarse_ref[...] = (coarse_in[...].astype(f32) + coarse).astype(bf16)
    fine_ref[...] = (fine_in[...].astype(f32) + fine).astype(bf16)


def product_kernel(coarse_ref, fine_ref, high_ref, low_ref, product_ref):
    coarse, high = coarse_ref[...], high_ref[...]
    product_ref[...] = nt(coarse, high) + (nt(fine_ref[...], high) + nt(coarse, low_ref[...]))


def residual_kernel(
    masks, samples, rank_ref, source_ref, x_ref, b_x_ref, d_x_ref, product_ref,
    features_ref, high_ref, low_ref, norm_ref, weights_ref, pivot_ref, residual_ref, send_ref,
):
    held, width = b_x_ref.shape
    source = source_of(source_ref)[1]
    new = ordered_x(source, held, b_x_ref) + ordered_x(source, 3 * held, d_x_ref)
    pivot_x = (new + x_ref[...].astype(f32)).astype(bf16)
    pivot_ref[...] = pivot_x
    high, low = high_ref[...], low_ref[...]
    pivot_wide = pivot_x.astype(f32)
    pivot_norm = jnp.sum(pivot_wide * pivot_wide, axis=1, keepdims=True)
    residual_ref[...] = (
        mixed(nt(pivot_x, features_ref[...]), pivot_norm, norm_ref[...], width) - product_ref[...]
    )
    core, _, order = spots(rank_ref[0], *masks)
    weights = weights_ref[...] / samples
    gram_half(residual_ref, 1 - core, weights, high, low, order, send_ref)


def keep_kernel(masks, samples, rank_ref, residual_ref, high_ref, low_ref, weights_ref, keep_ref):
    core, order, _ = spots(rank_ref[0], *masks)
    weights = weights_ref[...] / samples
    gram_half(residual_ref, core, weights, high_ref[...], low_ref[...], order, keep_ref)


def eliminate(work_ref, k):
    n = work_ref.shape[0]
    size = PANEL
    lane = iota((size, n), 1)
    row_wide = iota((size, n), 0)
    row = iota((size, 128), 0)
    first = pl.multiple_of(k * size, size)
    rows = work_ref[pl.ds(first, size), :]
    slab = rows[:, 0:128]
    for g in range(1, n // 128):
        slab = jnp.where(first >= g * 128, rows[:, g * 128 : (g + 1) * 128], slab)
    slab = pltpu.roll(slab, (128 - first % 128) % 128, 1)
    columns = [jnp.broadcast_to(slab[:, j : j + 1], (size, 128)) for j in range(size)]
    scale = jnp.zeros((size, 128), f32)
    for j in range(size):
        pivot = columns[j][j : j + 1, :]
        scale = jnp.where(row == j, lax.rsqrt(pivot), scale)
        factor = jnp.where(row > j, columns[j] * (1.0 / pivot), 0.0)
        for l in range(j + 1, size):
            columns[l] = columns[l] - factor * columns[l][j : j + 1, :]
        rows = jnp.where(lane == first + j, jnp.where(row_wide == j, 1.0, 0.0), rows)
        rows = rows - jnp.concatenate([factor] * (n // 128), axis=1) * rows[j : j + 1, :]
    rows = rows * jnp.concatenate([scale] * (n // 128), axis=1)
    upper = jnp.where(lane >= first + size, rows, 0.0)
    update = tn(upper, rows, HIGHEST)
    full_lane, full_row = iota((n, n), 1), iota((n, n), 0)
    stale = (full_row >= first + size) & (full_lane >= first) & (full_lane < first + size)
    work_ref[...] = jnp.where(stale, 0.0, work_ref[...]) - update
    work_ref[pl.ds(first, size), :] = rows


def inverse_kernel(start, stop):
    def kernel(*refs):
        work_ref = refs[-1]
        n = work_ref.shape[0]
        if start == 0:
            pivot_x, pivot_hi, pivot_lo = [ref[...] for ref in refs[:3]]
            width = pivot_x.shape[1]
            wide = pivot_x.astype(f32)
            square = wide * wide
            left = jnp.sum(square, axis=1, keepdims=True)
            right = nt(jnp.ones((8, width), f32), square, HIGHEST)[0:1, :]
            product = nt(pivot_hi, pivot_hi) + (nt(pivot_lo, pivot_hi) + nt(pivot_hi, pivot_lo))
            work_ref[...] = mixed(nt(pivot_x, pivot_x), left, right, width) - product
        else:
            work_ref[...] = refs[0][...]

        def panel(k, carry):
            eliminate(work_ref, k)
            return carry

        lax.fori_loop(start, stop, panel, 0)
        if stop == n // PANEL:
            work_ref[...] = jnp.where(iota((n, n), 1) <= iota((n, n), 0), work_ref[...], 0.0)

    return kernel


def columns_kernel(residual_ref, inverse_ref, out_ref):
    out_ref[...] = dot(residual_ref[...], inverse_ref[...], 0, 1, HIGHEST)


def rows_kernel(masks, rank_ref, *refs):
    inverse_ref, out_ref, work_ref, done_ref, sems = refs[-5:]
    parts = refs[:-5]
    count = len(parts) // 2
    piece = parts[0].shape[1]
    n = inverse_ref.shape[0]
    total = done_ref.shape[1]
    depth = total - n
    middle = n // 2
    core, near_order, far_order = spots(rank_ref[0], *masks)
    for k, part in enumerate(parts):
        mine = k < count
        half = core if mine else 1 - core
        at = half * count + ((near_order if mine else far_order) ^ (k % count))
        upper = pl.ds(pl.multiple_of(at * piece, piece), piece)
        lower = pl.ds(pl.multiple_of(middle + at * piece, piece), piece)
        work_ref[upper, 0:depth] = part[0, :, 0:depth]
        work_ref[lower, 0:depth] = part[0, :, depth : 2 * depth]
        work_ref[upper, depth:] = part[0, :, 2 * depth : 2 * depth + n]
        work_ref[lower, depth + middle :] = part[0, :, 2 * depth + n :]
    inverse = inverse_ref[...]
    corner = work_ref[0:middle, depth + middle :]
    first = nn(inverse[:, 0:middle], work_ref[0:middle, depth : depth + middle], HIGHEST) + nt(
        inverse[:, middle:], corner, HIGHEST
    )
    second = nn(inverse, work_ref[:, depth + middle :], HIGHEST)
    done_ref[:, depth:] = nt(jnp.concatenate([first, second], axis=1), inverse, HIGHEST)
    copies = []

    def send(here):
        copy = pltpu.make_async_copy(
            done_ref.at[:, here], out_ref.at[:, here], sems.at[len(copies)]
        )
        copies.append(copy)
        copy.start()

    send(slice(depth, total))
    for at in range(0, depth, depth // 4):
        here = slice(at, at + depth // 4)
        done_ref[:, here] = nn(inverse, work_ref[:, here], HIGHEST)
        send(here)
    for copy in copies:
        copy.wait()


def body(features, factor, ip_weights, pivot_owner, pivot_position):
    axes = ("row", "col")
    n_row, n_col = lax.axis_size("row"), lax.axis_size("col")
    devices = n_row * n_col
    row_bits, col_bits = n_row.bit_length() - 1, n_col.bit_length() - 1
    assert n_row == 1 << row_bits and n_col == 1 << col_bits and row_bits >= 2 and col_bits >= 1
    col_low = 1
    core = n_col
    side = 2 * n_col
    masks = (core, side, col_low)
    others = [n_col << k for k in range(2, row_bits)] + [1 << k for k in range(1, col_bits)]
    others = others[::-1]
    rank = (lax.axis_index("row") * n_col + lax.axis_index("col")).astype(i32)[None]
    pivots = pivot_owner.shape[0]
    slots = 2 * pivots // devices + 2
    rows, width = features.shape
    depth = factor.shape[1]
    samples = rows * devices
    total = depth + pivots

    def pair(mask):
        return [(i, i ^ mask) for i in range(devices)]

    def staggered(mask_zero, mask_one):
        return [(i, i ^ (mask_one if i & core else mask_zero)) for i in range(devices)]

    first_pair = staggered(side, col_low)
    second_pair = staggered(col_low, side)
    both_pair = pair(side | col_low)
    core_pair = pair(core)

    def move(value, perm):
        return lax.ppermute(value, axes, perm)

    def tie(*values):
        return lax.optimization_barrier(values)

    owner_row = pivot_owner[None, :]
    far = lambda x: pltpu.with_memory_space_constraint(x, pltpu.HBM)
    listed = (1, pivots)
    held_x, held_h, kept, factor_near = pl.pallas_call(
        pick_kernel,
        out_shape=(
            pltpu.VMEM((slots, width), bf16),
            pltpu.VMEM((slots, depth), jnp.int16),
            pltpu.VMEM((rows, width), bf16),
            pltpu.VMEM((rows, depth), f32),
        ),
        in_specs=[pl.BlockSpec(memory_space=pltpu.SMEM)] + [pl.BlockSpec(memory_space=pltpu.HBM)] * 4,
        out_specs=tuple(pl.BlockSpec(memory_space=pltpu.VMEM) for _ in range(4)),
        scratch_shapes=[
            pltpu.VMEM(listed, i32),
            pltpu.VMEM(listed, i32),
            pltpu.SMEM(listed, i32),
            pltpu.SMEM(listed, i32),
            pltpu.SMEM((slots + 1,), i32),
            pltpu.VMEM((slots, depth), f32),
            pltpu.SemaphoreType.DMA((7,)),
        ],
        compiler_params=pltpu.CompilerParams(vmem_limit_bytes=24 << 20),
    )(rank, far(owner_row), far(pivot_position[None, :]), far(features), far(factor))

    def joined(one, two):
        shape = (2 * one.shape[0], one.shape[1])
        return call(join_kernel, pltpu.VMEM(shape, one.dtype), one, two)

    prepared = False
    perms = [pair(mask) for mask in others] + [first_pair]
    perms_x = [pair(mask) for mask in others[::-1]] + [first_pair]
    for perm, perm_x in zip(perms, perms_x):
        got_h = near(move(held_h, perm))
        got_x = near(move(held_x, perm_x))
        if not prepared:
            source, norm, high, low = call(
                prepare_kernel(core, side, col_low, others, slots, devices),
                (
                    pltpu.VMEM((2, pivots), i32),
                    pltpu.VMEM((1, rows), f32),
                    pltpu.VMEM((rows, depth), bf16),
                    pltpu.VMEM((rows, depth), bf16),
                ),
                rank, owner_row, kept, factor_near, smem=1,
            )
            got_h, got_x, source, norm, high, low = tie(got_h, got_x, source, norm, high, low)
            prepared = True
        held_h = joined(held_h, got_h)
        held_x = joined(held_x, got_x)
    across_h = near(move(held_h, second_pair))
    across_x = near(move(held_x, second_pair))
    far_h, far_x = near(move(held_h, core_pair)), near(move(held_x, core_pair))
    plane = pltpu.VMEM((pivots, depth), bf16)
    pivot_x, coarse, fine = call(
        order_kernel,
        (pltpu.VMEM((pivots, width), bf16), plane, plane),
        source, held_x, held_h, far_x, far_h,
    )
    across_h, coarse, fine = tie(across_h, coarse, fine)
    beyond_h = near(move(across_h, core_pair))
    coarse, fine = call(partial(across_kernel, 1), (plane, plane), source, across_h, coarse, fine)
    coarse, fine = call(partial(across_kernel, 3), (plane, plane), source, beyond_h, coarse, fine)
    across_x, coarse, fine = tie(across_x, coarse, fine)
    beyond_x = near(move(across_x, core_pair))
    product = call(product_kernel, pltpu.VMEM((pivots, rows), f32), coarse, fine, high, low)
    beyond_x, product = tie(beyond_x, product)

    weights = ip_weights[None, :]
    half = pltpu.VMEM((4, pivots // 16, 2 * depth + pivots + pivots // 2), f32)
    pivot_x, residual, send = call(
        partial(residual_kernel, masks, samples),
        (pltpu.VMEM((pivots, width), bf16), pltpu.VMEM((pivots, rows), f32), half),
        rank, source, pivot_x, across_x, beyond_x, product, kept, high, low, norm, weights,
        smem=1,
    )
    received = move(send, core_pair)
    keep = call(partial(keep_kernel, masks, samples), half, rank, residual, high, low, weights, smem=1)
    keep = keep + received

    panels = pivots // PANEL
    cuts = [0, panels * 3 // 8, panels * 3 // 4, panels]

    def eliminate_step(step, *given):
        return call(
            inverse_kernel(cuts[step], cuts[step + 1]), pltpu.VMEM((pivots, pivots), f32), *given
        )

    keep, pivot_x, coarse, fine = tie(keep, pivot_x, coarse, fine)
    from_both = move(keep[3:4], both_pair)
    from_second = move(keep[1:2], second_pair)
    from_first = move(keep[2:3], first_pair)
    work = eliminate_step(0, pivot_x, coarse, fine)
    from_both, from_second, from_first, work = tie(from_both, from_second, from_first, work)
    keep = (keep[0:1] + from_both) + (from_second + from_first)
    step = 1
    split_at = keep.shape[1] // 2
    one, two = keep[:, :split_at], keep[:, split_at:]
    for mask, other_mask in zip(others, others[::-1]):
        got_one, got_two = move(one, pair(mask)), move(two, pair(other_mask))
        if step < len(cuts) - 1:
            work = eliminate_step(step, work)
            got_one, got_two, work = tie(got_one, got_two, work)
            step += 1
        one, two = one + got_one, two + got_two
    keep = jnp.concatenate([one, two], axis=1)
    inverse = work
    keep, inverse = tie(keep, inverse)
    pieces = [near(keep)] + [near(move(keep, perm)) for perm in (second_pair, first_pair, both_pair)]
    new_columns = call(columns_kernel, jax.ShapeDtypeStruct((rows, pivots), f32), residual, inverse)
    pieces[3], new_columns = tie(pieces[3], new_columns)
    pieces += [near(move(piece, core_pair)) for piece in pieces]
    gram_rows = pl.pallas_call(
        partial(rows_kernel, masks),
        out_shape=jax.ShapeDtypeStruct((pivots, total), f32),
        in_specs=[pl.BlockSpec(memory_space=pltpu.SMEM)] + [pl.BlockSpec(memory_space=pltpu.VMEM)] * 9,
        out_specs=pl.BlockSpec(memory_space=pltpu.HBM),
        scratch_shapes=[
            pltpu.VMEM((pivots, total), f32),
            pltpu.VMEM((pivots, total), f32),
            pltpu.SemaphoreType.DMA((5,)),
        ],
        compiler_params=pltpu.CompilerParams(vmem_limit_bytes=24 << 20),
    )(rank, *pieces, inverse)
    return (new_columns, gram_rows)


def solution(mesh):
    placed = (P(("row", "col"), None), P(("row", "col"), None), P(("row", "col")), P(), P())

    return jax.shard_map(
        body, mesh=mesh, in_specs=placed, out_specs=(P(("row", "col"), None), P()), check_vma=False
    )
```

```python
from functools import partial

import jax
import jax.numpy as jnp
from jax import lax
from jax.experimental import pallas as pl
from jax.experimental.pallas import tpu as pltpu
from jax.sharding import PartitionSpec as P


HIGHEST = lax.Precision.HIGHEST
f32 = jnp.float32
bf16 = jnp.bfloat16
i32 = jnp.int32
PANEL = 32
STEPS = 2.0**20


def dot(a, b, left, right, precision=None):
    return lax.dot_general(
        a, b, (((left,), (right,)), ((), ())), precision=precision, preferred_element_type=f32
    )


def nn(a, b, precision=None):
    return dot(a, b, 1, 0, precision)


def nt(a, b, precision=None):
    return dot(a, b, 1, 1, precision)


def tn(a, b, precision=None):
    return dot(a, b, 0, 0, precision)


def split(a):
    high = a.astype(bf16)
    low = (a - high.astype(f32)).astype(bf16)
    return high, low


def near(x):
    return pltpu.with_memory_space_constraint(x, pltpu.VMEM)


def call(kernel, outs, *args, smem=0, scratch=(), flops=10**9):
    specs = [pl.BlockSpec(memory_space=pltpu.SMEM)] * smem + [
        pl.BlockSpec(memory_space=pltpu.VMEM)
    ] * (len(args) - smem)
    return pl.pallas_call(
        kernel,
        out_shape=outs,
        in_specs=specs,
        out_specs=jax.tree.map(lambda _: pl.BlockSpec(memory_space=pltpu.VMEM), outs),
        scratch_shapes=scratch,
        compiler_params=pltpu.CompilerParams(vmem_limit_bytes=24 << 20),
        cost_estimate=pl.CostEstimate(flops=flops, transcendentals=0, bytes_accessed=10**6),
    )(*args)


def onehot(mask):
    return jnp.where(mask, 1.0, 0.0).astype(bf16)


def iota(shape, axis):
    return lax.broadcasted_iota(i32, shape, axis)


def pick_kernel(
    rank_ref, owner_ref, position_ref, features_ref, factor_ref,
    slots_x_ref, slots_h_ref, kept_ref, factor_in,
    owner_in, position_in, owner_list, position_list, found, rows_in, sems,
):
    slots = slots_x_ref.shape[0]
    pivots = owner_ref.shape[1]
    rows = features_ref.shape[0]
    half = rows // 2
    pairs = [
        (owner_ref, owner_list),
        (position_ref, position_list),
        (owner_ref, owner_in),
        (position_ref, position_in),
        (features_ref, kept_ref),
        (factor_ref.at[pl.ds(0, half), :], factor_in.at[pl.ds(0, half), :]),
        (factor_ref.at[pl.ds(half, half), :], factor_in.at[pl.ds(half, half), :]),
    ]
    copies = [
        pltpu.make_async_copy(source, target, sems.at[k]) for k, (source, target) in enumerate(pairs)
    ]
    for k in (0, 1, 2, 3, 5, 6, 4):
        copies[k].start()
    rank = rank_ref[0]
    for k in range(slots + 1):
        found[k] = 0
    copies[0].wait()
    copies[1].wait()

    def collect(k, count):
        for p in range(8):
            at = k * 8 + p
            found[count] = position_list[0, at]
            count = jnp.minimum(count + (owner_list[0, at] == rank).astype(i32), slots)
        return count

    lax.fori_loop(0, pivots // 8, collect, jnp.int32(0))
    ahead = onehot(iota((pivots, pivots), 0) < iota((pivots, pivots), 1))
    copies[2].wait()
    mine = owner_in[...] == rank
    mine_rows = jnp.broadcast_to(jnp.where(mine, 1.0, 0.0), (8, pivots)).astype(bf16)
    order = nn(mine_rows, ahead)[0:1, :].astype(i32)
    chosen = onehot((iota((slots, pivots), 0) == order) & mine)
    copies[3].wait()
    located = onehot(iota((rows, pivots), 0) == position_in[...])
    take = nt(chosen, located).astype(bf16)
    copies[4].wait()
    slots_x_ref[...] = nn(take, kept_ref[...]).astype(bf16)
    copies[5].wait()
    copies[6].wait()
    for k in range(slots):
        rows_in[k : k + 1, :] = factor_in[pl.ds(found[k], 1), :]
    slots_h_ref[...] = jnp.round(rows_in[...] * STEPS).astype(i32).astype(jnp.int16)


def prepare_kernel(core, side, col_low, others, slots, devices):
    def kernel(
        rank_ref, owner_ref, features_ref, factor_ref, source_ref, norm_ref, high_ref, low_ref
    ):
        pivots = owner_ref.shape[1]
        owner = owner_ref[...]
        ahead = onehot(iota((pivots, pivots), 0) < iota((pivots, pivots), 1))
        owned = iota((devices, pivots), 0) == owner
        counts = nn(onehot(owned), ahead)
        slot_rank = jnp.sum(jnp.where(owned, counts, 0.0), axis=0, keepdims=True).astype(i32)
        apart = owner ^ rank_ref[0]
        bit = lambda mask: (apart >> (mask.bit_length() - 1)) & 1
        at = len(others)
        low_core = (owner & core) == 0
        lead = jnp.where(low_core, bit(side), bit(col_low))
        trail = jnp.where(low_core, bit(col_low), bit(side))
        outer = (lead << at) + (trail << (at + 1)) + (bit(core) << (at + 2))
        for row, chain in enumerate((others, others[::-1])):
            place = outer
            for k, mask in enumerate(chain):
                place = place + (bit(mask) << k)
            source_ref[row : row + 1, :] = place * slots + slot_rank
        high, low = split(factor_ref[...])
        high_ref[...] = high
        low_ref[...] = low
        wide = features_ref[...].astype(f32)
        norm_ref[...] = nt(jnp.ones((8, wide.shape[1]), f32), wide * wide, HIGHEST)[0:1, :]

    return kernel


def mixed(cross, left, right, width):
    base = jnp.exp((left + right - 2.0 * cross) * (-0.25 / width))
    square = base * base
    return 0.5 * base + 0.3 * square + 0.2 * (square * square)


def join_kernel(*refs):
    out_ref = refs[-1]
    at = 0
    for ref in refs[:-1]:
        out_ref[at : at + ref.shape[0]] = ref[...]
        at += ref.shape[0]


def spots(rank, core, side, col_low):
    bit = lambda mask: (rank >> (mask.bit_length() - 1)) & 1
    lead = jnp.where(bit(core) == 0, bit(side), bit(col_low))
    trail = jnp.where(bit(core) == 0, bit(col_low), bit(side))
    return bit(core), lead * 2 + trail, trail * 2 + lead


def gram_half(residual_ref, half, weights, high, low, order, out_ref):
    count, piece, _ = out_ref.shape
    size = count * piece
    depth = high.shape[1]
    n = residual_ref.shape[0]
    upper = residual_ref[pl.ds(pl.multiple_of(half * size, size), size), :]
    lower = residual_ref[pl.ds(pl.multiple_of(n // 2 + half * size, size), size), :]
    weighted = jnp.concatenate([upper, lower], axis=0) * weights
    weighted_hi, weighted_lo = split(weighted)
    left = nn(weighted_hi, high) + (nn(weighted_lo, high) + nn(weighted_hi, low))
    residual = residual_ref[...]
    top = nt(weighted[0:size], residual, HIGHEST)
    bottom = nt(weighted[size:], residual[n // 2 :], HIGHEST)
    for p in range(count):
        spot = (order & (count - 1)) ^ p
        rows = slice(p * piece, (p + 1) * piece)
        out_ref[spot, :, 0:depth] = left[rows]
        out_ref[spot, :, depth : 2 * depth] = left[size + p * piece : size + (p + 1) * piece]
        out_ref[spot, :, 2 * depth : 2 * depth + n] = top[rows]
        out_ref[spot, :, 2 * depth + n :] = bottom[rows]


def chosen_rows(source, start, held):
    return onehot(iota((held, source.shape[1]), 0) == source - start)


def source_of(source_ref):
    return source_ref[0:1, :], source_ref[1:2, :]


def ordered_h(source, start, h_ref):
    chosen = chosen_rows(source, start, h_ref.shape[0])
    q = h_ref[...].astype(i32)
    coarse = (q + 128) >> 8
    fine = q - (coarse << 8)
    coarse = (coarse.astype(f32) * (256 / STEPS)).astype(bf16)
    fine = (fine.astype(f32) * (1 / STEPS)).astype(bf16)
    return tn(chosen, coarse), tn(chosen, fine)


def ordered_x(source, start, x_ref):
    return tn(chosen_rows(source, start, x_ref.shape[0]), x_ref[...])


def order_kernel(source_ref, a_x_ref, a_h_ref, c_x_ref, c_h_ref, x_ref, coarse_ref, fine_ref):
    held = a_x_ref.shape[0]
    source, source_x = source_of(source_ref)
    x_ref[...] = (
        ordered_x(source_x, 0, a_x_ref) + ordered_x(source_x, 2 * held, c_x_ref)
    ).astype(bf16)
    one, two = ordered_h(source, 0, a_h_ref), ordered_h(source, 2 * held, c_h_ref)
    coarse_ref[...] = (one[0] + two[0]).astype(bf16)
    fine_ref[...] = (one[1] + two[1]).astype(bf16)


def across_kernel(place, source_ref, h_ref, coarse_in, fine_in, coarse_ref, fine_ref):
    coarse, fine = ordered_h(source_of(source_ref)[0], place * h_ref.shape[0], h_ref)
    coarse_ref[...] = (coarse_in[...].astype(f32) + coarse).astype(bf16)
    fine_ref[...] = (fine_in[...].astype(f32) + fine).astype(bf16)


def product_kernel(coarse_ref, fine_ref, high_ref, low_ref, product_ref):
    coarse, high = coarse_ref[...], high_ref[...]
    product_ref[...] = nt(coarse, high) + (nt(fine_ref[...], high) + nt(coarse, low_ref[...]))


def residual_kernel(
    masks, samples, rank_ref, source_ref, x_ref, b_x_ref, d_x_ref, product_ref,
    features_ref, high_ref, low_ref, norm_ref, weights_ref, pivot_ref, residual_ref, send_ref,
):
    held, width = b_x_ref.shape
    source = source_of(source_ref)[1]
    new = ordered_x(source, held, b_x_ref) + ordered_x(source, 3 * held, d_x_ref)
    pivot_x = (new + x_ref[...].astype(f32)).astype(bf16)
    pivot_ref[...] = pivot_x
    high, low = high_ref[...], low_ref[...]
    pivot_wide = pivot_x.astype(f32)
    pivot_norm = jnp.sum(pivot_wide * pivot_wide, axis=1, keepdims=True)
    residual_ref[...] = (
        mixed(nt(pivot_x, features_ref[...]), pivot_norm, norm_ref[...], width) - product_ref[...]
    )
    core, _, order = spots(rank_ref[0], *masks)
    weights = weights_ref[...] / samples
    gram_half(residual_ref, 1 - core, weights, high, low, order, send_ref)


def keep_kernel(masks, samples, rank_ref, residual_ref, high_ref, low_ref, weights_ref, keep_ref):
    core, order, _ = spots(rank_ref[0], *masks)
    weights = weights_ref[...] / samples
    gram_half(residual_ref, core, weights, high_ref[...], low_ref[...], order, keep_ref)


def eliminate(work_ref, k):
    n = work_ref.shape[0]
    size = PANEL
    lane = iota((size, n), 1)
    row_wide = iota((size, n), 0)
    row = iota((size, 128), 0)
    first = pl.multiple_of(k * size, size)
    rows = work_ref[pl.ds(first, size), :]
    slab = rows[:, 0:128]
    for g in range(1, n // 128):
        slab = jnp.where(first >= g * 128, rows[:, g * 128 : (g + 1) * 128], slab)
    slab = pltpu.roll(slab, (128 - first % 128) % 128, 1)
    columns = [jnp.broadcast_to(slab[:, j : j + 1], (size, 128)) for j in range(size)]
    scale = jnp.zeros((size, 128), f32)
    for j in range(size):
        pivot = columns[j][j : j + 1, :]
        scale = jnp.where(row == j, lax.rsqrt(pivot), scale)
        factor = jnp.where(row > j, columns[j] * (1.0 / pivot), 0.0)
        for l in range(j + 1, size):
            columns[l] = columns[l] - factor * columns[l][j : j + 1, :]
        rows = jnp.where(lane == first + j, jnp.where(row_wide == j, 1.0, 0.0), rows)
        rows = rows - jnp.concatenate([factor] * (n // 128), axis=1) * rows[j : j + 1, :]
    rows = rows * jnp.concatenate([scale] * (n // 128), axis=1)
    upper = jnp.where(lane >= first + size, rows, 0.0)
    update = tn(upper, rows, HIGHEST)
    full_lane, full_row = iota((n, n), 1), iota((n, n), 0)
    stale = (full_row >= first + size) & (full_lane >= first) & (full_lane < first + size)
    work_ref[...] = jnp.where(stale, 0.0, work_ref[...]) - update
    work_ref[pl.ds(first, size), :] = rows


def inverse_kernel(start, stop):
    def kernel(*refs):
        work_ref = refs[-1]
        n = work_ref.shape[0]
        if start == 0:
            pivot_x, pivot_hi, pivot_lo = [ref[...] for ref in refs[:3]]
            width = pivot_x.shape[1]
            wide = pivot_x.astype(f32)
            square = wide * wide
            left = jnp.sum(square, axis=1, keepdims=True)
            right = nt(jnp.ones((8, width), f32), square, HIGHEST)[0:1, :]
            product = nt(pivot_hi, pivot_hi) + (nt(pivot_lo, pivot_hi) + nt(pivot_hi, pivot_lo))
            work_ref[...] = mixed(nt(pivot_x, pivot_x), left, right, width) - product
        else:
            work_ref[...] = refs[0][...]

        def panel(k, carry):
            eliminate(work_ref, k)
            return carry

        lax.fori_loop(start, stop, panel, 0)
        if stop == n // PANEL:
            work_ref[...] = jnp.where(iota((n, n), 1) <= iota((n, n), 0), work_ref[...], 0.0)

    return kernel


def columns_kernel(residual_ref, inverse_ref, out_ref):
    out_ref[...] = dot(residual_ref[...], inverse_ref[...], 0, 1, HIGHEST)


def rows_kernel(masks, rank_ref, *refs):
    inverse_ref, out_ref, work_ref, done_ref, sems = refs[-5:]
    parts = refs[:-5]
    count = len(parts) // 2
    piece = parts[0].shape[1]
    n = inverse_ref.shape[0]
    total = done_ref.shape[1]
    depth = total - n
    middle = n // 2
    core, near_order, far_order = spots(rank_ref[0], *masks)
    for k, part in enumerate(parts):
        mine = k < count
        half = core if mine else 1 - core
        at = half * count + ((near_order if mine else far_order) ^ (k % count))
        upper = pl.ds(pl.multiple_of(at * piece, piece), piece)
        lower = pl.ds(pl.multiple_of(middle + at * piece, piece), piece)
        work_ref[upper, 0:depth] = part[0, :, 0:depth]
        work_ref[lower, 0:depth] = part[0, :, depth : 2 * depth]
        work_ref[upper, depth:] = part[0, :, 2 * depth : 2 * depth + n]
        work_ref[lower, depth + middle :] = part[0, :, 2 * depth + n :]
    inverse = inverse_ref[...]
    corner = work_ref[0:middle, depth + middle :]
    first = nn(inverse[:, 0:middle], work_ref[0:middle, depth : depth + middle], HIGHEST) + nt(
        inverse[:, middle:], corner, HIGHEST
    )
    second = nn(inverse, work_ref[:, depth + middle :], HIGHEST)
    done_ref[:, depth:] = nt(jnp.concatenate([first, second], axis=1), inverse, HIGHEST)
    copies = []

    def send(here):
        copy = pltpu.make_async_copy(
            done_ref.at[:, here], out_ref.at[:, here], sems.at[len(copies)]
        )
        copies.append(copy)
        copy.start()

    send(slice(depth, total))
    inverse_hi, inverse_lo = split(inverse)
    for at in range(0, depth, depth // 4):
        here = slice(at, at + depth // 4)
        part_hi, part_lo = split(work_ref[:, here])
        done_ref[:, here] = nn(inverse_hi, part_hi) + (
            nn(inverse_lo, part_hi) + nn(inverse_hi, part_lo)
        )
        send(here)
    for copy in copies:
        copy.wait()


def body(features, factor, ip_weights, pivot_owner, pivot_position):
    axes = ("row", "col")
    n_row, n_col = lax.axis_size("row"), lax.axis_size("col")
    devices = n_row * n_col
    row_bits, col_bits = n_row.bit_length() - 1, n_col.bit_length() - 1
    assert n_row == 1 << row_bits and n_col == 1 << col_bits and row_bits >= 2 and col_bits >= 1
    col_low = 1
    core = n_col
    side = 2 * n_col
    masks = (core, side, col_low)
    others = [n_col << k for k in range(2, row_bits)] + [1 << k for k in range(1, col_bits)]
    others = others[::-1]
    rank = (lax.axis_index("row") * n_col + lax.axis_index("col")).astype(i32)[None]
    pivots = pivot_owner.shape[0]
    slots = 2 * pivots // devices + 2
    rows, width = features.shape
    depth = factor.shape[1]
    samples = rows * devices
    total = depth + pivots

    def pair(mask):
        return [(i, i ^ mask) for i in range(devices)]

    def staggered(mask_zero, mask_one):
        return [(i, i ^ (mask_one if i & core else mask_zero)) for i in range(devices)]

    first_pair = staggered(side, col_low)
    second_pair = staggered(col_low, side)
    both_pair = pair(side | col_low)
    core_pair = pair(core)

    def move(value, perm):
        return lax.ppermute(value, axes, perm)

    def tie(*values):
        return lax.optimization_barrier(values)

    owner_row = pivot_owner[None, :]
    far = lambda x: pltpu.with_memory_space_constraint(x, pltpu.HBM)
    listed = (1, pivots)
    held_x, held_h, kept, factor_near = pl.pallas_call(
        pick_kernel,
        out_shape=(
            pltpu.VMEM((slots, width), bf16),
            pltpu.VMEM((slots, depth), jnp.int16),
            pltpu.VMEM((rows, width), bf16),
            pltpu.VMEM((rows, depth), f32),
        ),
        in_specs=[pl.BlockSpec(memory_space=pltpu.SMEM)] + [pl.BlockSpec(memory_space=pltpu.HBM)] * 4,
        out_specs=tuple(pl.BlockSpec(memory_space=pltpu.VMEM) for _ in range(4)),
        scratch_shapes=[
            pltpu.VMEM(listed, i32),
            pltpu.VMEM(listed, i32),
            pltpu.SMEM(listed, i32),
            pltpu.SMEM(listed, i32),
            pltpu.SMEM((slots + 1,), i32),
            pltpu.VMEM((slots, depth), f32),
            pltpu.SemaphoreType.DMA((7,)),
        ],
        compiler_params=pltpu.CompilerParams(vmem_limit_bytes=24 << 20),
    )(rank, far(owner_row), far(pivot_position[None, :]), far(features), far(factor))

    def joined(one, two):
        shape = (2 * one.shape[0], one.shape[1])
        return call(join_kernel, pltpu.VMEM(shape, one.dtype), one, two)

    prepared = False
    perms = [pair(mask) for mask in others] + [first_pair]
    perms_x = [pair(mask) for mask in others[::-1]] + [first_pair]
    for perm, perm_x in zip(perms, perms_x):
        got_h = near(move(held_h, perm))
        got_x = near(move(held_x, perm_x))
        if not prepared:
            source, norm, high, low = call(
                prepare_kernel(core, side, col_low, others, slots, devices),
                (
                    pltpu.VMEM((2, pivots), i32),
                    pltpu.VMEM((1, rows), f32),
                    pltpu.VMEM((rows, depth), bf16),
                    pltpu.VMEM((rows, depth), bf16),
                ),
                rank, owner_row, kept, factor_near, smem=1,
            )
            got_h, got_x, source, norm, high, low = tie(got_h, got_x, source, norm, high, low)
            prepared = True
        held_h = joined(held_h, got_h)
        held_x = joined(held_x, got_x)
    across_h = near(move(held_h, second_pair))
    across_x = near(move(held_x, second_pair))
    far_h, far_x = near(move(held_h, core_pair)), near(move(held_x, core_pair))
    plane = pltpu.VMEM((pivots, depth), bf16)
    pivot_x, coarse, fine = call(
        order_kernel,
        (pltpu.VMEM((pivots, width), bf16), plane, plane),
        source, held_x, held_h, far_x, far_h,
    )
    across_h, coarse, fine = tie(across_h, coarse, fine)
    beyond_h = near(move(across_h, core_pair))
    coarse, fine = call(partial(across_kernel, 1), (plane, plane), source, across_h, coarse, fine)
    coarse, fine = call(partial(across_kernel, 3), (plane, plane), source, beyond_h, coarse, fine)
    across_x, coarse, fine = tie(across_x, coarse, fine)
    beyond_x = near(move(across_x, core_pair))
    product = call(product_kernel, pltpu.VMEM((pivots, rows), f32), coarse, fine, high, low)
    beyond_x, product = tie(beyond_x, product)

    weights = ip_weights[None, :]
    half = pltpu.VMEM((4, pivots // 16, 2 * depth + pivots + pivots // 2), f32)
    pivot_x, residual, send = call(
        partial(residual_kernel, masks, samples),
        (pltpu.VMEM((pivots, width), bf16), pltpu.VMEM((pivots, rows), f32), half),
        rank, source, pivot_x, across_x, beyond_x, product, kept, high, low, norm, weights,
        smem=1,
    )
    received = move(send, core_pair)
    keep = call(partial(keep_kernel, masks, samples), half, rank, residual, high, low, weights, smem=1)
    keep = keep + received

    panels = pivots // PANEL
    cuts = [0, panels // 2, panels * 3 // 4, panels]

    def eliminate_step(step, *given):
        return call(
            inverse_kernel(cuts[step], cuts[step + 1]), pltpu.VMEM((pivots, pivots), f32), *given
        )

    keep, pivot_x, coarse, fine = tie(keep, pivot_x, coarse, fine)
    from_both = move(keep[3:4], both_pair)
    from_second = move(keep[1:2], second_pair)
    from_first = move(keep[2:3], first_pair)
    work = eliminate_step(0, pivot_x, coarse, fine)
    from_both, from_second, from_first, work = tie(from_both, from_second, from_first, work)
    keep = (keep[0:1] + from_both) + (from_second + from_first)
    step = 1
    split_at = keep.shape[1] // 2
    one, two = keep[:, :split_at], keep[:, split_at:]
    for mask, other_mask in zip(others, others[::-1]):
        got_one, got_two = move(one, pair(mask)), move(two, pair(other_mask))
        if step < len(cuts) - 1:
            work = eliminate_step(step, work)
            got_one, got_two, work = tie(got_one, got_two, work)
            step += 1
        one, two = one + got_one, two + got_two
    keep = jnp.concatenate([one, two], axis=1)
    inverse = work
    keep, inverse = tie(keep, inverse)
    pieces = [near(keep)] + [near(move(keep, perm)) for perm in (second_pair, first_pair, both_pair)]
    new_columns = call(columns_kernel, jax.ShapeDtypeStruct((rows, pivots), f32), residual, inverse)
    pieces[3], new_columns = tie(pieces[3], new_columns)
    pieces += [near(move(piece, core_pair)) for piece in pieces]
    gram_rows = pl.pallas_call(
        partial(rows_kernel, masks),
        out_shape=jax.ShapeDtypeStruct((pivots, total), f32),
        in_specs=[pl.BlockSpec(memory_space=pltpu.SMEM)] + [pl.BlockSpec(memory_space=pltpu.VMEM)] * 9,
        out_specs=pl.BlockSpec(memory_space=pltpu.HBM),
        scratch_shapes=[
            pltpu.VMEM((pivots, total), f32),
            pltpu.VMEM((pivots, total), f32),
            pltpu.SemaphoreType.DMA((5,)),
        ],
        compiler_params=pltpu.CompilerParams(vmem_limit_bytes=24 << 20),
    )(rank, *pieces, inverse)
    return (new_columns, gram_rows)


def solution(mesh):
    placed = (P(("row", "col"), None), P(("row", "col"), None), P(("row", "col")), P(), P())

    return jax.shard_map(
        body, mesh=mesh, in_specs=placed, out_specs=(P(("row", "col"), None), P()), check_vma=False
    )
```
